32 devices in a mesh: dp: 8 (over y, x, core), mp: 4 (over z).
Axes of the slice: x: 2, y: 2, z: 4, core: 2. Of those that a mesh axis runs over, the one named last changes fastest.
Arguments:
- candidates: bfloat16 [64, 256, 768], P('dp', 'mp'), may hold values from -6 to 6
- owner_row: int32 [64], replicated, may hold values from 0 to 63, as said below
- selected: int32 [16], replicated, may hold values from 0 to 63, as said below
- dest_slot: int32 [16], replicated, may hold values from 0 to 15, as said below
- patch_weight: bfloat16 [768, 768], P(None, 'mp'), may hold values from -0.21875 to 0.21875
- positions: bfloat16 [256, 768], P(None, 'mp'), may hold values from -3 to 3
- qkv_weight: bfloat16 [768, 3, 768], P(None, None, 'mp'), may hold values from -1 to 1
- out_weight: bfloat16 [768, 768], P('mp'), may hold values from -0.21875 to 0.21875
- attn_gain: bfloat16 [768], replicated, may hold values from 0.099609375 to 1.8984375
- mlp_gain: bfloat16 [768], replicated, may hold values from 0.099609375 to 1.8984375
- up_weight: bfloat16 [768, 3072], P(None, 'mp'), may hold values from -0.21875 to 0.21875
- down_weight: bfloat16 [3072, 768], P('mp'), may hold values from -0.109375 to 0.109375
Outputs:
- layer_out: bfloat16 [16, 256, 768], P('dp', 'mp')
The draws below stay inside these ranges and needn't reach their ends.
Inputs may be any that keep to these rules, and one draw needn't show every extreme that they name: `owner_row`: a permutation; storage row r sits on index r // 8 of dp. `selected`: distinct candidates; no index of dp stores more than 4 of them, and some index stores exactly 4. `dest_slot`: a permutation; the 2 slots s with equal s // 2 get candidates stored on different indices of dp.
All inputs are finite; a program needn't handle non-finite values.
Results may differ from the reference program's by a relative error of at most 0.012.
Values may be sent and summed in bfloat16 or wider, within the bound.
No kernel may reach another device: no remote copies, remote signals or barrier semaphores. Data moves between devices by JAX's collectives and lax.ppermute only.
A program may use at most 128 MiB of HBM per device.

```python
import math
import jax
import jax.numpy as jnp
from jax import lax

D = 768
HEADS = 12
FF = 3072
PIX = 768
PATCHES = 256
CAND_DEV = 8
SEL_DEV = 2
MOST = 4
HEAD_DIM = 64
CANDS = 64
SEL = 16
N_MP = 4


def routing_plan(key):
    subkeys = jax.random.split(jax.random.fold_in(key, 41), 5)
    learners = SEL // SEL_DEV
    owner_row = jax.random.permutation(subkeys[0], CANDS).astype(jnp.int32)
    placing = jax.random.permutation(subkeys[1], learners).astype(jnp.int32)
    position = jnp.argsort(placing).astype(jnp.int32)
    group_index = position // MOST
    within = position % MOST
    counts = jnp.where(group_index % 2 == 0, jnp.where(within < SEL_DEV, MOST, 0), SEL_DEV).astype(jnp.int32)
    run_end = jnp.cumsum(counts).astype(jnp.int32)
    starts = run_end - counts
    series = jnp.arange(SEL, dtype=jnp.int32)
    owners = jnp.sum((run_end[None, :] <= series[:, None]).astype(jnp.int32), axis=1).astype(jnp.int32)
    local_rank = series - starts[owners]
    shuffles = jax.vmap(lambda sub: jax.random.permutation(sub, CAND_DEV))(jax.random.split(subkeys[2], learners)).astype(jnp.int32)
    storage = owners * CAND_DEV + shuffles[owners, local_rank]
    inverse = jnp.argsort(owner_row).astype(jnp.int32)
    chosen = inverse[storage]
    learner_order = jax.random.permutation(subkeys[3], learners).astype(jnp.int32)
    slot_index = learner_order[series % learners] * SEL_DEV + series // learners
    mixing = jax.random.permutation(subkeys[4], SEL).astype(jnp.int32)
    return (owner_row, chosen[mixing].astype(jnp.int32), slot_index[mixing].astype(jnp.int32))


def draw_owner_row(key, part):
    return routing_plan(key)[0]


def draw_selected(key, part):
    return routing_plan(key)[1]


def draw_dest_slot(key, part):
    return routing_plan(key)[2]


def draw_qkv_weight(key, part):
    base = jax.random.normal(key, (D, 3, D), jnp.float32) / math.sqrt(D)
    return jnp.clip(base, -1.0, 1.0).astype(jnp.bfloat16)


def level_of(stream_key, dims, shards, least, high):
    loudness = 1.0
    for axis_at, shards_of in shards:
        steps = jax.random.uniform(jax.random.fold_in(jax.random.fold_in(stream_key, 6), axis_at), (shards_of,), jnp.float32, least / len(shards), high / len(shards))
        loudness = loudness * jnp.repeat(jnp.exp(steps), dims[axis_at] // shards_of).reshape((-1,) + (1,) * (len(dims) - 1 - axis_at))
    return loudness


def normal_values(own_key, shape, scale, most, cuts=(), held_as=jnp.bfloat16):
    result = jax.random.normal(own_key, shape, jnp.float32) * scale
    if len(cuts) > 0:
        result = level_of(own_key, shape, cuts, -0.22, 0.18) * result
    return jnp.clip(result, min=-most, max=most).astype(held_as)


def setup_inputs(seed: int = 0) -> dict:
    key_of = jax.random.split(jax.random.key(seed), 13)
    return {
        "candidates": normal_values(key_of[0], (CANDS, PATCHES, PIX), 1.0, 6.0, ((0, 8), (1, 4))),
        "owner_row": draw_owner_row(jax.random.fold_in(key_of[12], 71), 0),
        "selected": draw_selected(jax.random.fold_in(key_of[12], 71), 0),
        "dest_slot": draw_dest_slot(jax.random.fold_in(key_of[12], 71), 0),
        "patch_weight": normal_values(key_of[4], (PIX, D), PIX ** -0.5, 0.21875, ((1, 4),)),
        "positions": normal_values(key_of[5], (PATCHES, D), 0.5, 3.0, ((1, 4),)),
        "qkv_weight": draw_qkv_weight(jax.random.fold_in(key_of[12], 71), 0),
        "out_weight": normal_values(key_of[7], (D, D), D ** -0.5, 0.21875, ((0, 4),)),
        "attn_gain": jnp.clip(1.0 + 0.18 * jax.random.normal(key_of[8], (D,), jnp.float32), 0.099609375, 1.8984375).astype(jnp.bfloat16),
        "mlp_gain": jnp.clip(1.0 + 0.18 * jax.random.normal(key_of[9], (D,), jnp.float32), 0.099609375, 1.8984375).astype(jnp.bfloat16),
        "up_weight": normal_values(key_of[10], (D, FF), D ** -0.5, 0.21875, ((1, 4),)),
        "down_weight": normal_values(key_of[11], (FF, D), FF ** -0.5, 0.109375, ((0, 4),)),
    }


def norm_rows(values, gain):
    average = lax.optimization_barrier(jnp.mean(values, axis=-1, keepdims=True))
    centred = values - average
    variance = lax.optimization_barrier(jnp.mean(centred * centred, axis=-1, keepdims=True))
    return centred * lax.rsqrt(variance + 1e-06) * gain.astype(jnp.float32)

def group_sum(left, right, groups):
    count = left.shape[0]
    left_groups = left.reshape(count, groups, left.shape[1] // groups).astype(jnp.float32)
    right_groups = right.reshape(groups, right.shape[0] // groups, right.shape[1]).astype(jnp.float32)
    partials = jnp.einsum('tgk,gkd->tgd', left_groups, right_groups)
    rounded = lax.optimization_barrier(partials.astype(jnp.bfloat16))
    return lax.optimization_barrier(jnp.sum(rounded.astype(jnp.float32), axis=1))

def layer_one(pixels, patch_weight, positions, qkv_weight, out_weight, attn_gain, mlp_gain, up_weight, down_weight):
    embedded = (jnp.dot(pixels, patch_weight, preferred_element_type=jnp.float32) + positions.astype(jnp.float32)).astype(jnp.bfloat16)
    activations = embedded.astype(jnp.float32)
    normed = norm_rows(activations, attn_gain).astype(jnp.bfloat16)
    projected = jnp.einsum('td,dce->tce', normed.astype(jnp.float32), qkv_weight.astype(jnp.float32)).astype(jnp.bfloat16)
    head_split = projected.reshape(PATCHES, 3, HEADS, HEAD_DIM).astype(jnp.float32)
    queries = head_split[:, 0]
    attn_keys = head_split[:, 1]
    attn_values = head_split[:, 2]
    scores = jnp.einsum('qhd,khd->hqk', queries, attn_keys) * HEAD_DIM ** (-0.5)
    attn_probs = jax.nn.softmax(scores, axis=-1).astype(jnp.bfloat16)
    context = jnp.einsum('hqk,khd->qhd', attn_probs.astype(jnp.float32), attn_values).astype(jnp.bfloat16)
    context = context.reshape(PATCHES, D)
    attended = group_sum(context, out_weight, N_MP)
    after_attn = activations + attended
    normed2 = norm_rows(after_attn, mlp_gain).astype(jnp.bfloat16)
    hidden = jax.nn.gelu(jnp.dot(normed2, up_weight, preferred_element_type=jnp.float32), approximate=False).astype(jnp.bfloat16)
    feed = group_sum(hidden, down_weight, N_MP)
    return (after_attn + feed).astype(jnp.bfloat16)

def reference(candidates, owner_row, selected, dest_slot, patch_weight, positions, qkv_weight, out_weight, attn_gain, mlp_gain, up_weight, down_weight):
    chosen_rows = jnp.take(owner_row, selected).astype(jnp.int32)
    slot_rows = jnp.zeros((SEL,), jnp.int32).at[dest_slot].set(chosen_rows)
    batch = jnp.take(candidates, slot_rows, axis=0)

    def one_example(pixels):
        return layer_one(pixels, patch_weight, positions, qkv_weight, out_weight, attn_gain, mlp_gain, up_weight, down_weight)
    return lax.map(one_example, batch)
```

```python
import jax
import jax.numpy as jnp
from jax import lax
from jax.sharding import PartitionSpec as P

CAND_DEV = 8
SEL_DEV = 2
HEAD_DIM = 64


def norm_rows(values, gain):
    average = jnp.mean(values, axis=-1, keepdims=True)
    centred = values - average
    variance = jnp.mean(centred * centred, axis=-1, keepdims=True)
    return centred * lax.rsqrt(variance + 1e-06) * gain.astype(jnp.float32)


def shift(value, step):
    count = lax.axis_size("mp")
    return lax.ppermute(value, "mp", [(i, (i + step) % count) for i in range(count)])


def spread(value):
    return [value] + [shift(value, s) for s in range(1, lax.axis_size("mp"))]


def collect(parts):
    return [parts[0]] + [shift(parts[s], -s) for s in range(1, lax.axis_size("mp"))]


def total(parts):
    result = parts[0].astype(jnp.float32)
    for part in parts[1:]:
        result = result + part.astype(jnp.float32)
    return result


def local(
    candidates,
    owner_row,
    selected,
    dest_slot,
    patch_weight,
    positions,
    qkv_weight,
    out_weight,
    attn_gain,
    mlp_gain,
    up_weight,
    down_weight,
):
    learners = lax.axis_size("dp")
    own_index = lax.axis_index("dp")
    groups = lax.axis_size("mp")
    own_group = lax.axis_index("mp")
    quarter = candidates.shape[1]
    pixel_width = candidates.shape[2]
    chosen_rows = jnp.take(owner_row, selected)
    slot_rows = jnp.zeros(dest_slot.shape, jnp.int32).at[dest_slot].set(chosen_rows)
    source_owner = slot_rows // CAND_DEV
    local_row = slot_rows % CAND_DEV
    mine = (source_owner == own_index).reshape(learners, SEL_DEV)
    picked = jnp.sum(jnp.where(mine, local_row.reshape(learners, SEL_DEV), 0), axis=1)
    outgoing = jnp.take(candidates, picked, axis=0)
    incoming = lax.all_to_all(outgoing, "dp", split_axis=0, concat_axis=0, tiled=True)
    senders = lax.dynamic_slice_in_dim(source_owner, own_index * SEL_DEV, SEL_DEV)
    own_pixels = jnp.take(incoming, senders, axis=0)

    weight_parts = [patch_weight]
    position_parts = [lax.dynamic_slice_in_dim(positions, own_group * quarter, quarter, 0)]
    for s in range(1, groups):
        rows = lax.dynamic_slice_in_dim(positions, ((own_group + s) % groups) * quarter, quarter, 0)
        both = shift(jnp.concatenate([patch_weight, rows], axis=0), s)
        weight_parts.append(both[:pixel_width])
        position_parts.append(both[pixel_width:])
    stack = jnp.stack(
        [jnp.concatenate([w, p], axis=0) for w, p in zip(weight_parts, position_parts)]
    )
    whole = jnp.concatenate(
        [
            lax.dynamic_index_in_dim(stack, (own_group - j) % groups, 0, keepdims=False)
            for j in range(groups)
        ],
        axis=1,
    )
    product = jnp.einsum(
        "brp,pe->bre", own_pixels, whole[:pixel_width], preferred_element_type=jnp.float32
    )
    embedded = (product + whole[pixel_width:].astype(jnp.float32)[None]).astype(jnp.bfloat16)
    activations = embedded.astype(jnp.float32)
    normed = norm_rows(activations, attn_gain).astype(jnp.bfloat16)
    tokens = jnp.concatenate(spread(normed), axis=1)
    projected = jnp.einsum(
        "btd,dce->btce", tokens, qkv_weight, preferred_element_type=jnp.float32
    ).astype(jnp.bfloat16)
    local_heads = qkv_weight.shape[2] // HEAD_DIM
    head_split = projected.reshape(SEL_DEV, groups * quarter, 3, local_heads, HEAD_DIM)
    queries = head_split[:, :, 0]
    attn_keys = head_split[:, :, 1]
    attn_values = head_split[:, :, 2]
    scores = jnp.einsum(
        "bqhd,bkhd->bhqk", queries, attn_keys, preferred_element_type=jnp.float32
    ) * HEAD_DIM ** (-0.5)
    attn_probs = jax.nn.softmax(scores, axis=-1).astype(jnp.bfloat16)
    context = jnp.einsum(
        "bhqk,bkhd->bqhd", attn_probs, attn_values, preferred_element_type=jnp.float32
    ).astype(jnp.bfloat16)
    context = context.reshape(SEL_DEV, groups * quarter, local_heads * HEAD_DIM)
    partial_out = jnp.einsum(
        "bte,ed->btd", context, out_weight, preferred_element_type=jnp.float32
    ).astype(jnp.bfloat16)
    attended = total(
        collect([partial_out[:, s * quarter : (s + 1) * quarter] for s in range(groups)])
    )
    after_attn = activations + attended
    normed2 = norm_rows(after_attn, mlp_gain).astype(jnp.bfloat16)
    down_terms = []
    for part in spread(normed2):
        hidden = jax.nn.gelu(
            jnp.einsum("btd,df->btf", part, up_weight, preferred_element_type=jnp.float32),
            approximate=False,
        ).astype(jnp.bfloat16)
        down_terms.append(
            jnp.einsum(
                "btf,fd->btd", hidden, down_weight, preferred_element_type=jnp.float32
            ).astype(jnp.bfloat16)
        )
    return (after_attn + total(collect(down_terms))).astype(jnp.bfloat16)


def solution(mesh):
    return jax.shard_map(
        local,
        mesh=mesh,
        in_specs=(
            P("dp", "mp", None),
            P(),
            P(),
            P(),
            P(None, "mp"),
            P(None, "mp"),
            P(None, None, "mp"),
            P("mp", None),
            P(),
            P(),
            P(None, "mp"),
            P("mp", None),
        ),
        out_specs=P("dp", "mp", None),
        check_vma=False,
    )
```

```python
import jax
import jax.numpy as jnp
from jax import lax
from jax.sharding import PartitionSpec as P

CAND_DEV = 8
SEL_DEV = 2
HEAD_DIM = 64


def norm_rows(values, gain):
    average = jnp.mean(values, axis=-1, keepdims=True)
    centred = values - average
    variance = jnp.mean(centred * centred, axis=-1, keepdims=True)
    return centred * lax.rsqrt(variance + 1e-06) * gain.astype(jnp.float32)


def shift(value, step):
    count = lax.axis_size("mp")
    return lax.ppermute(value, "mp", [(i, (i + step) % count) for i in range(count)])


def far_first(count):
    return sorted(range(1, count), key=lambda s: (-min(s, count - s), -s))


def exchange(parts, sign):
    count = lax.axis_size("mp")
    results = [parts[0]] + [None] * (count - 1)
    for s in far_first(count):
        results[s] = shift(parts[s], s * sign)
    return results


def spread(value):
    return exchange([value] * lax.axis_size("mp"), 1)


def collect(parts):
    return exchange(parts, -1)


def total(parts):
    result = parts[0].astype(jnp.float32)
    for part in parts[1:]:
        result = result + part.astype(jnp.float32)
    return result


def layer(
    candidates,
    owner_row,
    selected,
    dest_slot,
    patch_weight,
    positions,
    qkv_weight,
    out_weight,
    attn_gain,
    mlp_gain,
    up_weight,
    down_weight,
):
    learners = lax.axis_size("dp")
    own_index = lax.axis_index("dp")
    groups = lax.axis_size("mp")
    own_group = lax.axis_index("mp")
    quarter = candidates.shape[1]
    pixel_width = candidates.shape[2]
    chosen_rows = jnp.take(owner_row, selected)
    slot_rows = jnp.zeros(dest_slot.shape, jnp.int32).at[dest_slot].set(chosen_rows)
    source_owner = slot_rows // CAND_DEV
    local_row = slot_rows % CAND_DEV
    mine = (source_owner == own_index).reshape(learners, SEL_DEV)
    picked = jnp.sum(jnp.where(mine, local_row.reshape(learners, SEL_DEV), 0), axis=1)
    outgoing = jnp.take(candidates, picked, axis=0)
    incoming = lax.all_to_all(outgoing, "dp", split_axis=0, concat_axis=0, tiled=True)
    senders = lax.dynamic_slice_in_dim(source_owner, own_index * SEL_DEV, SEL_DEV)
    own_pixels = jnp.take(incoming, senders, axis=0)

    bundles = []
    for s in range(groups):
        rows = lax.dynamic_slice_in_dim(positions, ((own_group + s) % groups) * quarter, quarter, 0)
        bundles.append(jnp.concatenate([patch_weight, rows], axis=0))
    stack = jnp.stack(exchange(bundles, 1))
    whole = jnp.concatenate(
        [
            lax.dynamic_index_in_dim(stack, (own_group - j) % groups, 0, keepdims=False)
            for j in range(groups)
        ],
        axis=1,
    )
    product = jnp.einsum(
        "brp,pe->bre", own_pixels, whole[:pixel_width], preferred_element_type=jnp.float32
    )
    embedded = (product + whole[pixel_width:].astype(jnp.float32)[None]).astype(jnp.bfloat16)
    activations = embedded.astype(jnp.float32)
    normed = norm_rows(activations, attn_gain).astype(jnp.bfloat16)
    tokens = jnp.concatenate(spread(normed), axis=1)
    projected = jnp.einsum(
        "btd,dce->btce", tokens, qkv_weight, preferred_element_type=jnp.float32
    ).astype(jnp.bfloat16)
    local_heads = qkv_weight.shape[2] // HEAD_DIM
    head_split = projected.reshape(SEL_DEV, groups * quarter, 3, local_heads, HEAD_DIM)
    queries = head_split[:, :, 0]
    attn_keys = head_split[:, :, 1]
    attn_values = head_split[:, :, 2]
    scores = jnp.einsum(
        "bqhd,bkhd->bhqk", queries, attn_keys, preferred_element_type=jnp.float32
    ) * HEAD_DIM ** (-0.5)
    attn_probs = jax.nn.softmax(scores, axis=-1).astype(jnp.bfloat16)
    context = jnp.einsum(
        "bhqk,bkhd->bqhd", attn_probs, attn_values, preferred_element_type=jnp.float32
    ).astype(jnp.bfloat16)
    context = context.reshape(SEL_DEV, groups * quarter, local_heads * HEAD_DIM)
    partial_out = jnp.einsum(
        "bte,ed->btd", context, out_weight, preferred_element_type=jnp.float32
    ).astype(jnp.bfloat16)
    attended = total(
        collect([partial_out[:, s * quarter : (s + 1) * quarter] for s in range(groups)])
    )
    after_attn = activations + attended
    normed2 = norm_rows(after_attn, mlp_gain).astype(jnp.bfloat16)
    tokens2 = jnp.concatenate(spread(normed2), axis=1)
    hidden = jax.nn.gelu(
        jnp.einsum("btd,df->btf", tokens2, up_weight, preferred_element_type=jnp.float32),
        approximate=False,
    ).astype(jnp.bfloat16)
    down_terms = jnp.einsum(
        "btf,fd->btd", hidden, down_weight, preferred_element_type=jnp.float32
    ).astype(jnp.bfloat16)
    feed = total(collect([down_terms[:, s * quarter : (s + 1) * quarter] for s in range(groups)]))
    return (after_attn + feed).astype(jnp.bfloat16)


def solution(mesh):
    return jax.shard_map(
        layer,
        mesh=mesh,
        in_specs=(
            P("dp", "mp", None),
            P(),
            P(),
            P(),
            P(None, "mp"),
            P(None, "mp"),
            P(None, None, "mp"),
            P("mp", None),
            P(),
            P(),
            P(None, "mp"),
            P("mp", None),
        ),
        out_specs=P("dp", "mp", None),
        check_vma=False,
    )
```

```python
import jax
import jax.numpy as jnp
from jax import lax
from jax.experimental import pallas as pl
from jax.experimental.pallas import tpu as pltpu
from jax.sharding import PartitionSpec as P

CAND_DEV = 8
SEL_DEV = 2
HEAD_DIM = 64
SPREAD = 8
BF16 = jnp.bfloat16
F32 = jnp.float32


def norm_rows(values, gain):
    average = jnp.mean(values, axis=-1, keepdims=True)
    centred = values - average
    variance = jnp.mean(centred * centred, axis=-1, keepdims=True)
    return centred * lax.rsqrt(variance + 1e-06) * gain.astype(F32)


def swap(value, axis, bits):
    return lax.ppermute(value, axis, [(i, i ^ bits) for i in range(lax.axis_size(axis))])


def dot(left, right):
    return jnp.dot(left, right, preferred_element_type=F32)


ANY = pl.BlockSpec(memory_space=pl.ANY)
SCALARS = pl.BlockSpec(memory_space=pltpu.SMEM)
FAST = pl.BlockSpec(memory_space=pltpu.VMEM)
UNIT = 128
SMALL = pltpu.CompilerParams(vmem_limit_bytes=4 * 1024 * 1024)


def copier(body, outs, where, *operands):
    return pl.pallas_call(
        body,
        in_specs=[SCALARS] + [FAST] * len(operands),
        out_specs=tuple(FAST for _ in outs),
        out_shape=tuple(pltpu.VMEM(shape, BF16) for shape in outs),
        compiler_params=SMALL,
    )(where, *(pltpu.with_memory_space_constraint(x, pltpu.VMEM) for x in operands))


def route_kernel(own, owner_row, selected, dest_slot, candidates, outgoing, senders, sem):
    me = own[0]

    def visit(i, sent):
        row = owner_row[selected[i]]
        owner = row // CAND_DEV
        slot = dest_slot[i]

        @pl.when(slot // SEL_DEV == me)
        def _():
            senders[slot % SEL_DEV] = owner

        @pl.when(owner == me)
        def _():
            pltpu.make_async_copy(
                candidates.at[row % CAND_DEV], outgoing.at[slot // SEL_DEV], sem.at[0]
            ).start()

        return sent + (owner == me).astype(jnp.int32)

    sent = lax.fori_loop(0, selected.shape[0], visit, 0)

    def finish(_, carry):
        pltpu.make_async_copy(candidates.at[0], outgoing.at[0], sem.at[0]).wait()
        return carry

    lax.fori_loop(0, sent, finish, 0)


def route(owner_row, selected, dest_slot, candidates):
    learners = lax.axis_size("dp")
    own = jnp.full((1,), lax.axis_index("dp"), jnp.int32)
    return pl.pallas_call(
        route_kernel,
        in_specs=[SCALARS] * 4 + [ANY],
        out_specs=(FAST, SCALARS),
        out_shape=(
            jax.ShapeDtypeStruct((learners,) + candidates.shape[1:], BF16),
            jax.ShapeDtypeStruct((SEL_DEV,), jnp.int32),
        ),
        scratch_shapes=[pltpu.SemaphoreType.DMA((1,))],
    )(own, owner_row, selected, dest_slot, candidates)


def attn_unit(array, unit):
    columns = array.shape[1] // UNIT
    rows = array.shape[0] // 4
    return (
        pl.ds(pl.multiple_of((unit // columns) * rows, rows), rows),
        pl.ds(pl.multiple_of((unit % columns) * UNIT, UNIT), UNIT),
    )


def lanes(index):
    return pl.ds(pl.multiple_of(index * UNIT, UNIT), UNIT)


def block(index, size):
    return pl.ds(pl.multiple_of(index * size, size), size)


def extract_kernel(where, embed, attn, up, down, embed_piece, both_piece, mlp_piece, sem):
    piece = where[0]
    rows = embed.shape[0]
    size = up.shape[0] // SPREAD
    copies = [
        pltpu.make_async_copy(up.at[block(piece, size)], mlp_piece.at[pl.ds(0, size)], sem.at[0]),
        pltpu.make_async_copy(
            down.at[block(piece, size)], mlp_piece.at[pl.ds(size, size)], sem.at[1]
        ),
    ]
    for copy in copies:
        copy.start()
    unit = embed[:, lanes(piece)]
    embed_piece[...] = unit
    both_piece[:rows] = unit
    for i in range(3):
        both_piece[(1 + i) * rows : (2 + i) * rows] = attn[attn_unit(attn, 3 * piece + i)]
    for copy in copies:
        copy.wait()


def extract(where, embed, attn, up, down):
    rows = embed.shape[0]
    return pl.pallas_call(
        extract_kernel,
        in_specs=[SCALARS, FAST, FAST, ANY, ANY],
        out_specs=(FAST, FAST, FAST),
        out_shape=(
            pltpu.VMEM((rows, UNIT), BF16),
            pltpu.VMEM((4 * rows, UNIT), BF16),
            pltpu.VMEM((2 * up.shape[0] // SPREAD, up.shape[1]), BF16),
        ),
        scratch_shapes=[pltpu.SemaphoreType.DMA((2,))],
        compiler_params=SMALL,
    )(
        where,
        pltpu.with_memory_space_constraint(embed, pltpu.VMEM),
        pltpu.with_memory_space_constraint(attn, pltpu.VMEM),
        up,
        down,
    )


def units_kernel(where, neighbour, opposite, third, target):
    rows = neighbour.shape[0]
    target[:rows] = neighbour[...]
    target[rows : 2 * rows] = opposite[:rows]
    target[2 * rows : 3 * rows] = third[...]
    target[3 * rows :] = opposite[rows:]


def stack_kernel(where, *refs):
    *parts, target = refs
    rows = parts[0].shape[0]
    for n, part in enumerate(parts):
        target[n * rows : (n + 1) * rows] = part[...]


def place_attn_kernel(where, embed, mine, others, embed_whole, attn_far):
    piece, group = where[0], where[1]
    rows = embed.shape[0]
    size = 6 * rows
    embed_whole[block(group, rows)] = embed[...]
    for source, core in ((mine, 0), (others, 1)):
        for n in range(SPREAD // 2):
            p = piece ^ (2 * n + core)
            for k in range(3):
                at = n * size + k * rows
                embed_whole[block(group ^ (k + 1), rows), lanes(p)] = source[at : at + rows]
                at += 3 * rows
                attn_far[attn_unit(attn_far, 3 * p + k)] = source[at : at + rows]


def place_mlp_kernel(where, mine, others, up_far, down_far):
    piece = where[0]
    size = up_far.shape[0] // SPREAD
    for source, core in ((mine, 0), (others, 1)):
        for n in range(SPREAD // 2):
            p = piece ^ (2 * n + core)
            at = n * 2 * size
            up_far[block(p, size)] = source[at : at + size]
            down_far[block(p, size)] = source[at + size : at + 2 * size]


def neighbours_of(where, piece):
    parts = [piece]
    for bits in range(2, SPREAD, 2):
        parts.append(swap(piece, "dp", bits))
    rows = len(parts) * piece.shape[0]
    mine = copier(stack_kernel, ((rows,) + piece.shape[1:],), where, *parts)[0]
    return mine, swap(mine, "dp", 1)


def heads(projected, local_heads):
    return projected.reshape(projected.shape[0], local_heads, HEAD_DIM)


def attend(normed, shard):
    width = shard.shape[0] // 4
    qkv = shard[: 3 * width].reshape(3, width, -1)
    local_heads = width // HEAD_DIM
    projected = jnp.einsum("td,ced->cte", normed, qkv, preferred_element_type=F32).astype(BF16)
    queries, attn_keys, attn_values = (heads(projected[c], local_heads) for c in range(3))
    scores = jnp.einsum("qhd,khd->hqk", queries, attn_keys, preferred_element_type=F32)
    probs = jax.nn.softmax(scores * HEAD_DIM ** (-0.5), axis=-1).astype(BF16)
    context = jnp.einsum("hqk,khd->qhd", probs, attn_values, preferred_element_type=F32)
    return dot(context.astype(BF16).reshape(normed.shape[0], -1), shard[3 * width :])


def feed_forward(normed, up, down):
    hidden = jax.nn.gelu(dot(normed, up), approximate=False).astype(BF16)
    return dot(hidden, down)


def layer(
    candidates,
    owner_row,
    selected,
    dest_slot,
    patch_weight,
    positions,
    qkv_weight,
    out_weight,
    attn_gain,
    mlp_gain,
    up_weight,
    down_weight,
):
    groups = lax.axis_size("mp")
    group = lax.axis_index("mp")
    pair = group // 2
    quarter = candidates.shape[1]
    where = jnp.stack([lax.axis_index("dp") % SPREAD, group]).astype(jnp.int32)

    outgoing, senders = route(owner_row, selected, dest_slot, candidates)
    incoming = lax.all_to_all(outgoing, "dp", split_axis=0, concat_axis=0, tiled=True)

    patch_weight, positions, qkv_weight, out_weight, _ = lax.optimization_barrier(
        (patch_weight, positions, qkv_weight, out_weight, senders)
    )
    pixel_width, width = patch_weight.shape
    model = out_weight.shape[1]
    embed_own = jnp.concatenate([patch_weight.T, positions.T], axis=1)
    attn_own = jnp.concatenate([qkv_weight.transpose(1, 2, 0).reshape(-1, model), out_weight])
    embed_piece, both_piece, mlp_piece = extract(where, embed_own, attn_own, up_weight, down_weight)
    third = swap(embed_piece, "mp", 3)
    opposite = swap(both_piece, "mp", 2)
    neighbour = swap(embed_piece, "mp", 1)
    units = copier(units_kernel, ((6 * width, UNIT),), where, neighbour, opposite, third)[0]
    embed_whole, attn_far = copier(
        place_attn_kernel,
        ((groups * width, pixel_width + positions.shape[0]), attn_own.shape),
        where,
        embed_own,
        *neighbours_of(where, units),
    )
    mlp_piece = swap(mlp_piece, "mp", 2)
    up_far, down_far = copier(
        place_mlp_kernel,
        (up_weight.shape, down_weight.shape),
        where,
        *neighbours_of(where, mlp_piece),
    )

    kept = lax.dynamic_index_in_dim(incoming, senders[pair], 0, keepdims=False)
    given = lax.dynamic_index_in_dim(incoming, senders[1 - pair], 0, keepdims=False)
    third = swap(given, "mp", 3)
    opposite = swap(given, "mp", 2)
    neighbour = swap(kept, "mp", 1)
    pixels = jnp.concatenate([kept, opposite, neighbour, third])
    tokens = jnp.arange(groups * quarter, dtype=jnp.int32)
    block_of = tokens // quarter
    turned = (block_of >> 1) + 2 * (block_of & 1)
    spot = (group ^ turned) * quarter + tokens % quarter
    picks = (spot[:, None] == tokens[None, :]).astype(BF16)
    embedded = jnp.einsum(
        "tp,ep->te",
        jnp.concatenate([pixels, picks], axis=1),
        embed_whole,
        preferred_element_type=F32,
    ).astype(BF16)
    half = 2 * quarter
    normed = norm_rows(embedded.astype(F32), attn_gain).astype(BF16)
    attended = attend(normed, attn_own) + attend(normed, attn_far)
    other = swap(attended[half:].astype(BF16), "mp", 1)
    after_attn = embedded[:half].astype(F32) + (attended[:half] + other.astype(F32))
    normed2 = norm_rows(after_attn, mlp_gain).astype(BF16)
    tokens2 = jnp.concatenate([normed2, swap(normed2, "mp", 1)])
    feed = feed_forward(tokens2, up_weight, down_weight) + feed_forward(tokens2, up_far, down_far)
    blocks = [feed[i * quarter : (i + 1) * quarter] for i in range(4)]
    from_third = swap(blocks[3].astype(BF16), "mp", 3)
    from_opposite = swap((after_attn[quarter:] + blocks[1]).astype(BF16), "mp", 2)
    from_neighbour = swap(blocks[2].astype(BF16), "mp", 1)
    kept_out = (after_attn[:quarter] + (blocks[0] + from_neighbour.astype(F32))).astype(BF16)
    given_out = (from_opposite.astype(F32) + from_third.astype(F32)).astype(BF16)
    swapped = pair == 1
    return jnp.stack(
        [jnp.where(swapped, given_out, kept_out), jnp.where(swapped, kept_out, given_out)]
    )


def solution(mesh):
    return jax.shard_map(
        layer,
        mesh=mesh,
        in_specs=(
            P("dp", "mp", None),
            P(),
            P(),
            P(),
            P(None, "mp"),
            P(None, "mp"),
            P(None, None, "mp"),
            P("mp", None),
            P(),
            P(),
            P(None, "mp"),
            P("mp", None),
        ),
        out_specs=P("dp", "mp", None),
        check_vma=False,
    )
```

```python
import jax
import jax.numpy as jnp
from jax import lax
from jax.experimental import pallas as pl
from jax.experimental.pallas import tpu as pltpu
from jax.sharding import PartitionSpec as P

CAND_DEV = 8
SEL_DEV = 2
HEAD_DIM = 64
SPREAD = 8
BF16 = jnp.bfloat16
F32 = jnp.float32


def norm_rows(values, gain):
    average = jnp.mean(values, axis=-1, keepdims=True)
    centred = values - average
    variance = jnp.mean(centred * centred, axis=-1, keepdims=True)
    return centred * lax.rsqrt(variance + 1e-06) * gain.astype(F32)


def swap(value, axis, bits):
    return lax.ppermute(value, axis, [(i, i ^ bits) for i in range(lax.axis_size(axis))])


def dot(left, right):
    return jnp.dot(left, right, preferred_element_type=F32)


ANY = pl.BlockSpec(memory_space=pl.ANY)
SCALARS = pl.BlockSpec(memory_space=pltpu.SMEM)
FAST = pl.BlockSpec(memory_space=pltpu.VMEM)
UNIT = 128
SMALL = pltpu.CompilerParams(vmem_limit_bytes=4 * 1024 * 1024)


def copier(body, outs, where, *operands):
    return pl.pallas_call(
        body,
        in_specs=[SCALARS] + [FAST] * len(operands),
        out_specs=tuple(FAST for _ in outs),
        out_shape=tuple(pltpu.VMEM(shape, BF16) for shape in outs),
        compiler_params=SMALL,
    )(where, *(pltpu.with_memory_space_constraint(x, pltpu.VMEM) for x in operands))


def route_kernel(own, owner_row, selected, dest_slot, candidates, outgoing, senders, sem):
    me = own[0]

    def visit(i, sent):
        row = owner_row[selected[i]]
        owner = row // CAND_DEV
        slot = dest_slot[i]

        @pl.when(slot // SEL_DEV == me)
        def _():
            senders[slot % SEL_DEV] = owner

        @pl.when(owner == me)
        def _():
            pltpu.make_async_copy(
                candidates.at[row % CAND_DEV], outgoing.at[slot // SEL_DEV], sem.at[0]
            ).start()

        return sent + (owner == me).astype(jnp.int32)

    sent = lax.fori_loop(0, selected.shape[0], visit, 0)

    def finish(_, carry):
        pltpu.make_async_copy(candidates.at[0], outgoing.at[0], sem.at[0]).wait()
        return carry

    lax.fori_loop(0, sent, finish, 0)


def route(owner_row, selected, dest_slot, candidates):
    learners = lax.axis_size("dp")
    own = jnp.full((1,), lax.axis_index("dp"), jnp.int32)
    return pl.pallas_call(
        route_kernel,
        in_specs=[SCALARS] * 4 + [ANY],
        out_specs=(FAST, SCALARS),
        out_shape=(
            jax.ShapeDtypeStruct((learners,) + candidates.shape[1:], BF16),
            jax.ShapeDtypeStruct((SEL_DEV,), jnp.int32),
        ),
        scratch_shapes=[pltpu.SemaphoreType.DMA((1,))],
    )(own, owner_row, selected, dest_slot, candidates)


def attn_unit(array, unit):
    columns = array.shape[1] // UNIT
    rows = array.shape[0] // 4
    return (
        pl.ds(pl.multiple_of((unit // columns) * rows, rows), rows),
        pl.ds(pl.multiple_of((unit % columns) * UNIT, UNIT), UNIT),
    )


def lanes(index):
    return pl.ds(pl.multiple_of(index * UNIT, UNIT), UNIT)


def block(index, size):
    return pl.ds(pl.multiple_of(index * size, size), size)


def extract_kernel(where, embed, attn, up, down, embed_piece, both_piece, mlp_piece, sem):
    piece = where[0]
    rows = embed.shape[0]
    size = up.shape[0] // SPREAD
    copies = [
        pltpu.make_async_copy(up.at[block(piece, size)], mlp_piece.at[pl.ds(0, size)], sem.at[0]),
        pltpu.make_async_copy(
            down.at[block(piece, size)], mlp_piece.at[pl.ds(size, size)], sem.at[1]
        ),
    ]
    for copy in copies:
        copy.start()
    unit = embed[:, lanes(piece)]
    embed_piece[...] = unit
    both_piece[:rows] = unit
    for i in range(3):
        both_piece[(1 + i) * rows : (2 + i) * rows] = attn[attn_unit(attn, 3 * piece + i)]
    for copy in copies:
        copy.wait()


def extract(where, embed, attn, up, down):
    rows = embed.shape[0]
    return pl.pallas_call(
        extract_kernel,
        in_specs=[SCALARS, FAST, FAST, ANY, ANY],
        out_specs=(FAST, FAST, FAST),
        out_shape=(
            pltpu.VMEM((rows, UNIT), BF16),
            pltpu.VMEM((4 * rows, UNIT), BF16),
            pltpu.VMEM((2 * up.shape[0] // SPREAD, up.shape[1]), BF16),
        ),
        scratch_shapes=[pltpu.SemaphoreType.DMA((2,))],
        compiler_params=SMALL,
    )(
        where,
        pltpu.with_memory_space_constraint(embed, pltpu.VMEM),
        pltpu.with_memory_space_constraint(attn, pltpu.VMEM),
        up,
        down,
    )


def units_kernel(where, neighbour, opposite, third, target):
    rows = neighbour.shape[0]
    target[:rows] = neighbour[...]
    target[rows : 2 * rows] = opposite[:rows]
    target[2 * rows : 3 * rows] = third[...]
    target[3 * rows :] = opposite[rows:]


def stack_kernel(where, *refs):
    *parts, target = refs
    rows = parts[0].shape[0]
    for n, part in enumerate(parts):
        target[n * rows : (n + 1) * rows] = part[...]


def place_attn_kernel(where, embed, mine, others, embed_whole, attn_far):
    piece, group = where[0], where[1]
    rows = embed.shape[0]
    size = 6 * rows
    embed_whole[block(group, rows)] = embed[...]
    for source, core in ((mine, 0), (others, 1)):
        for n in range(SPREAD // 2):
            p = piece ^ (2 * n + core)
            for k in range(3):
                at = n * size + k * rows
                embed_whole[block(group ^ (k + 1), rows), lanes(p)] = source[at : at + rows]
                at += 3 * rows
                attn_far[attn_unit(attn_far, 3 * p + k)] = source[at : at + rows]


def place_mlp_kernel(where, mine, others, up_far, down_far):
    piece = where[0]
    size = up_far.shape[0] // SPREAD
    for source, core in ((mine, 0), (others, 1)):
        for n in range(SPREAD // 2):
            p = piece ^ (2 * n + core)
            at = n * 2 * size
            up_far[block(p, size)] = source[at : at + size]
            down_far[block(p, size)] = source[at + size : at + 2 * size]


def neighbours_of(where, piece):
    parts = [piece]
    for bits in range(2, SPREAD, 2):
        parts.append(swap(piece, "dp", bits))
    rows = len(parts) * piece.shape[0]
    mine = copier(stack_kernel, ((rows,) + piece.shape[1:],), where, *parts)[0]
    return mine, swap(mine, "dp", 1)


def turned_dot(left, right):
    return lax.dot_general(left, right, (((1,), (1,)), ((), ())), preferred_element_type=F32)


def columns_dot(left, right):
    return lax.dot_general(left, right, (((0,), (0,)), ((), ())), preferred_element_type=F32)


def context_of(normed, shard):
    width = shard.shape[0] // 4
    projected = turned_dot(shard[: 3 * width], normed).astype(BF16)
    results = []
    for at in range(0, width, HEAD_DIM):
        queries, attn_keys, attn_values = (
            projected[c * width + at : c * width + at + HEAD_DIM] for c in range(3)
        )
        scores = columns_dot(attn_keys, queries) * HEAD_DIM ** (-0.5)
        raised = jnp.exp(scores - jnp.max(scores, axis=0, keepdims=True))
        probs = (raised / jnp.sum(raised, axis=0, keepdims=True)).astype(BF16)
        results.append(dot(attn_values, probs).astype(BF16))
    return results


def attend_kernel(where, kept, opposite, neighbour, third, embed, own, far, gain, mine, other):
    group = where[1]
    quarter, pixel_width = kept.shape
    count = embed.shape[1] - pixel_width
    pixels = jnp.concatenate([kept[...], opposite[...], neighbour[...], third[...]], axis=0)
    row = lax.broadcasted_iota(jnp.int32, (count, count), 0)
    column = lax.broadcasted_iota(jnp.int32, (count, count), 1)
    block_of = row // quarter
    turned = (block_of >> 1) + 2 * (block_of & 1)
    spot = (turned ^ group) * quarter + row % quarter
    picks = jnp.where(spot == column, 1.0, 0.0).astype(BF16)
    product = turned_dot(pixels, embed[:, :pixel_width]) + turned_dot(picks, embed[:, pixel_width:])
    activations = product.astype(BF16).astype(F32)
    normed = norm_rows(activations, gain[...]).astype(BF16)
    width = own.shape[0] // 4
    context = jnp.concatenate(context_of(normed, own) + context_of(normed, far), axis=0)
    out = jnp.concatenate([own[3 * width :], far[3 * width :]], axis=0)
    attended = columns_dot(context, out)
    half = 2 * quarter
    mine[...] = activations[:half] + attended[:half]
    other[...] = attended[half:].astype(BF16)


def attend(where, parts, embed, own, far, gain):
    half = 2 * parts[0].shape[0]
    model = own.shape[1]
    held = [pltpu.with_memory_space_constraint(x, pltpu.VMEM) for x in (*parts, embed, own, far)]
    return pl.pallas_call(
        attend_kernel,
        in_specs=[SCALARS] + [FAST] * 8,
        out_specs=(FAST, FAST),
        out_shape=(pltpu.VMEM((half, model), F32), pltpu.VMEM((half, model), BF16)),
        compiler_params=pltpu.CompilerParams(vmem_limit_bytes=20 * 1024 * 1024),
    )(where, *held, gain.reshape(1, -1))


def gelu(values):
    return 0.5 * values * (1.0 + lax.erf(values * 0.5 ** 0.5))


def feed_through(normed, up, down):
    return dot(gelu(dot(normed, up)).astype(BF16), down)


def first_kernel(normed, up_far, down_far, up, down, feed, up_own, down_own, sem):
    copies = [
        pltpu.make_async_copy(up, up_own, sem.at[0]),
        pltpu.make_async_copy(down, down_own, sem.at[1]),
    ]
    for copy in copies:
        copy.start()
    part = feed_through(normed[...], up_far[...], down_far[...])
    for copy in copies:
        copy.wait()
    feed[...] = part + feed_through(normed[...], up_own[...], down_own[...])


def feed_first(normed, up_far, down_far, up, down):
    held = [pltpu.with_memory_space_constraint(x, pltpu.VMEM) for x in (normed, up_far, down_far)]
    return pl.pallas_call(
        first_kernel,
        in_specs=[FAST, FAST, FAST, ANY, ANY],
        out_specs=(FAST, FAST, FAST),
        out_shape=(
            pltpu.VMEM((normed.shape[0], down.shape[1]), F32),
            pltpu.VMEM(up.shape, BF16),
            pltpu.VMEM(down.shape, BF16),
        ),
        scratch_shapes=[pltpu.SemaphoreType.DMA((2,))],
        compiler_params=pltpu.CompilerParams(vmem_limit_bytes=16 * 1024 * 1024),
    )(*held, up, down)


def second_kernel(normed, up_far, down_far, up_own, down_own, near, third):
    part = feed_through(normed[...], up_far[...], down_far[...])
    part = part + feed_through(normed[...], up_own[...], down_own[...])
    quarter = near.shape[0]
    near[...] = part[:quarter].astype(BF16)
    third[...] = part[quarter:].astype(BF16)


def feed_second(*operands):
    half, model = operands[0].shape
    held = [pltpu.with_memory_space_constraint(x, pltpu.VMEM) for x in operands]
    return pl.pallas_call(
        second_kernel,
        in_specs=[FAST] * 5,
        out_specs=(FAST, FAST),
        out_shape=(pltpu.VMEM((half // 2, model), BF16), pltpu.VMEM((half // 2, model), BF16)),
        compiler_params=pltpu.CompilerParams(vmem_limit_bytes=16 * 1024 * 1024),
    )(*held)


def layer(
    candidates,
    owner_row,
    selected,
    dest_slot,
    patch_weight,
    positions,
    qkv_weight,
    out_weight,
    attn_gain,
    mlp_gain,
    up_weight,
    down_weight,
):
    groups = lax.axis_size("mp")
    group = lax.axis_index("mp")
    pair = group // 2
    quarter = candidates.shape[1]
    where = jnp.stack([lax.axis_index("dp") % SPREAD, group]).astype(jnp.int32)

    outgoing, senders = route(owner_row, selected, dest_slot, candidates)
    incoming = lax.all_to_all(outgoing, "dp", split_axis=0, concat_axis=0, tiled=True)

    patch_weight, positions, qkv_weight, out_weight, _ = lax.optimization_barrier(
        (patch_weight, positions, qkv_weight, out_weight, senders)
    )
    pixel_width, width = patch_weight.shape
    model = out_weight.shape[1]
    embed_own = jnp.concatenate([patch_weight.T, positions.T], axis=1)
    attn_own = jnp.concatenate([qkv_weight.transpose(1, 2, 0).reshape(-1, model), out_weight])
    embed_piece, both_piece, mlp_piece = extract(where, embed_own, attn_own, up_weight, down_weight)
    third = swap(embed_piece, "mp", 3)
    opposite = swap(both_piece, "mp", 2)
    neighbour = swap(embed_piece, "mp", 1)
    units = copier(units_kernel, ((6 * width, UNIT),), where, neighbour, opposite, third)[0]
    embed_whole, attn_far = copier(
        place_attn_kernel,
        ((groups * width, pixel_width + positions.shape[0]), attn_own.shape),
        where,
        embed_own,
        *neighbours_of(where, units),
    )
    mlp_piece = swap(mlp_piece, "mp", 2)
    up_far, down_far = copier(
        place_mlp_kernel,
        (up_weight.shape, down_weight.shape),
        where,
        *neighbours_of(where, mlp_piece),
    )

    kept = lax.dynamic_index_in_dim(incoming, senders[pair], 0, keepdims=False)
    given = lax.dynamic_index_in_dim(incoming, senders[1 - pair], 0, keepdims=False)
    third = swap(given, "mp", 3)
    opposite = swap(given, "mp", 2)
    neighbour = swap(kept, "mp", 1)
    mine, other = attend(
        where, (kept, opposite, neighbour, third), embed_whole, attn_own, attn_far, attn_gain
    )
    other = swap(other, "mp", 1)
    after_attn = mine + other.astype(F32)
    normed2 = norm_rows(after_attn, mlp_gain).astype(BF16)
    neighbour2 = swap(normed2, "mp", 1)
    feed, up_own, down_own = feed_first(normed2, up_far, down_far, up_weight, down_weight)
    from_opposite = swap((after_attn + feed)[quarter:].astype(BF16), "mp", 2)
    for_near, for_third = feed_second(neighbour2, up_far, down_far, up_own, down_own)
    from_third = swap(for_third, "mp", 3)
    from_neighbour = swap(for_near, "mp", 1)
    kept_out = (after_attn[:quarter] + (feed[:quarter] + from_neighbour.astype(F32))).astype(BF16)
    given_out = (from_opposite.astype(F32) + from_third.astype(F32)).astype(BF16)
    swapped = pair == 1
    return jnp.stack(
        [jnp.where(swapped, given_out, kept_out), jnp.where(swapped, kept_out, given_out)]
    )


def solution(mesh):
    return jax.shard_map(
        layer,
        mesh=mesh,
        in_specs=(
            P("dp", "mp", None),
            P(),
            P(),
            P(),
            P(None, "mp"),
            P(None, "mp"),
            P(None, None, "mp"),
            P("mp", None),
            P(),
            P(),
            P(None, "mp"),
            P("mp", None),
        ),
        out_specs=P("dp", "mp", None),
        check_vma=False,
    )
```

```python
import jax
import jax.numpy as jnp
from jax import lax
from jax.experimental import pallas as pl
from jax.experimental.pallas import tpu as pltpu
from jax.sharding import PartitionSpec as P

CAND_DEV = 8
SEL_DEV = 2
HEAD_DIM = 64
SPREAD = 8
BF16 = jnp.bfloat16
F32 = jnp.float32


def norm_rows(values, gain):
    average = jnp.mean(values, axis=-1, keepdims=True)
    centred = values - average
    variance = jnp.mean(centred * centred, axis=-1, keepdims=True)
    return centred * lax.rsqrt(variance + 1e-06) * gain.astype(F32)


def swap(value, axis, bits):
    return lax.ppermute(value, axis, [(i, i ^ bits) for i in range(lax.axis_size(axis))])


def dot(left, right):
    return jnp.dot(left, right, preferred_element_type=F32)


ANY = pl.BlockSpec(memory_space=pl.ANY)
SCALARS = pl.BlockSpec(memory_space=pltpu.SMEM)
FAST = pl.BlockSpec(memory_space=pltpu.VMEM)
SLOW = pl.BlockSpec(memory_space=pltpu.HBM)
UNIT = 128
SMALL = pltpu.CompilerParams(vmem_limit_bytes=4 * 1024 * 1024)


def copier(body, outs, where, *operands):
    return pl.pallas_call(
        body,
        in_specs=[SCALARS] + [FAST] * len(operands),
        out_specs=tuple(FAST for _ in outs),
        out_shape=tuple(pltpu.VMEM(shape, BF16) for shape in outs),
        compiler_params=SMALL,
    )(where, *(pltpu.with_memory_space_constraint(x, pltpu.VMEM) for x in operands))


def route_kernel(own, owner_row, selected, dest_slot, candidates, outgoing, senders, sem):
    me = own[0]

    def visit(i, sent):
        row = owner_row[selected[i]]
        owner = row // CAND_DEV
        slot = dest_slot[i]

        @pl.when(slot // SEL_DEV == me)
        def _():
            senders[slot % SEL_DEV] = owner

        @pl.when(owner == me)
        def _():
            pltpu.make_async_copy(
                candidates.at[row % CAND_DEV], outgoing.at[slot // SEL_DEV], sem.at[0]
            ).start()

        return sent + (owner == me).astype(jnp.int32)

    sent = lax.fori_loop(0, selected.shape[0], visit, 0)

    def finish(_, carry):
        pltpu.make_async_copy(candidates.at[0], outgoing.at[0], sem.at[0]).wait()
        return carry

    lax.fori_loop(0, sent, finish, 0)


def route(owner_row, selected, dest_slot, candidates):
    learners = lax.axis_size("dp")
    own = jnp.full((1,), lax.axis_index("dp"), jnp.int32)
    return pl.pallas_call(
        route_kernel,
        in_specs=[SCALARS] * 4 + [ANY],
        out_specs=(FAST, SCALARS),
        out_shape=(
            jax.ShapeDtypeStruct((learners,) + candidates.shape[1:], BF16),
            jax.ShapeDtypeStruct((SEL_DEV,), jnp.int32),
        ),
        scratch_shapes=[pltpu.SemaphoreType.DMA((1,))],
        compiler_params=pltpu.CompilerParams(vmem_limit_bytes=24 * 1024 * 1024),
    )(own, owner_row, selected, dest_slot, candidates)


def choose_kernel(where, senders, incoming, kept, given, sem):
    pair = where[1] // 2
    copies = [
        pltpu.make_async_copy(incoming.at[senders[pair]], kept, sem.at[0]),
        pltpu.make_async_copy(incoming.at[senders[1 - pair]], given, sem.at[1]),
    ]
    for copy in copies:
        copy.start()
    for copy in copies:
        copy.wait()


def choose(where, senders, incoming):
    shape = incoming.shape[1:]
    return pl.pallas_call(
        choose_kernel,
        in_specs=[SCALARS, SCALARS, SLOW],
        out_specs=(FAST, FAST),
        out_shape=(pltpu.VMEM(shape, BF16), pltpu.VMEM(shape, BF16)),
        scratch_shapes=[pltpu.SemaphoreType.DMA((2,))],
        compiler_params=SMALL,
    )(where, senders, pltpu.with_memory_space_constraint(incoming, pltpu.HBM))


def widen_kernel(values, wide):
    wide[...] = values[...].astype(F32)


def widen(values):
    row = values.reshape(1, -1)
    return pl.pallas_call(
        widen_kernel,
        in_specs=[FAST],
        out_specs=FAST,
        out_shape=jax.ShapeDtypeStruct(row.shape, F32),
        compiler_params=SMALL,
    )(row)


def attn_unit(array, unit):
    columns = array.shape[1] // UNIT
    rows = array.shape[0] // 4
    return (
        pl.ds(pl.multiple_of((unit // columns) * rows, rows), rows),
        pl.ds(pl.multiple_of((unit % columns) * UNIT, UNIT), UNIT),
    )


def lanes(index):
    return pl.ds(pl.multiple_of(index * UNIT, UNIT), UNIT)


def block(index, size):
    return pl.ds(pl.multiple_of(index * size, size), size)


def extract_kernel(where, embed, attn, up, down, embed_piece, both_piece, mlp_piece, sem):
    piece = where[0]
    rows = embed.shape[0]
    size = up.shape[0] // SPREAD
    copies = [
        pltpu.make_async_copy(up.at[block(piece, size)], mlp_piece.at[pl.ds(0, size)], sem.at[0]),
        pltpu.make_async_copy(
            down.at[block(piece, size)], mlp_piece.at[pl.ds(size, size)], sem.at[1]
        ),
    ]
    for copy in copies:
        copy.start()
    unit = embed[:, lanes(piece)]
    embed_piece[...] = unit
    both_piece[:rows] = unit
    for i in range(3):
        both_piece[(1 + i) * rows : (2 + i) * rows] = attn[attn_unit(attn, 3 * piece + i)]
    for copy in copies:
        copy.wait()


def extract(where, embed, attn, up, down):
    rows = embed.shape[0]
    return pl.pallas_call(
        extract_kernel,
        in_specs=[SCALARS, FAST, FAST, SLOW, SLOW],
        out_specs=(FAST, FAST, FAST),
        out_shape=(
            pltpu.VMEM((rows, UNIT), BF16),
            pltpu.VMEM((4 * rows, UNIT), BF16),
            pltpu.VMEM((2 * up.shape[0] // SPREAD, up.shape[1]), BF16),
        ),
        scratch_shapes=[pltpu.SemaphoreType.DMA((2,))],
        compiler_params=SMALL,
    )(
        where,
        pltpu.with_memory_space_constraint(embed, pltpu.VMEM),
        pltpu.with_memory_space_constraint(attn, pltpu.VMEM),
        pltpu.with_memory_space_constraint(up, pltpu.HBM),
        pltpu.with_memory_space_constraint(down, pltpu.HBM),
    )


def units_kernel(where, neighbour, opposite, third, target):
    rows = neighbour.shape[0]
    target[:rows] = neighbour[...]
    target[rows : 2 * rows] = opposite[:rows]
    target[2 * rows : 3 * rows] = third[...]
    target[3 * rows :] = opposite[rows:]


def stack_kernel(where, *refs):
    *parts, target = refs
    rows = parts[0].shape[0]
    for n, part in enumerate(parts):
        target[n * rows : (n + 1) * rows] = part[...]


def place_attn_kernel(where, embed, mine, others, embed_whole, attn_far):
    piece, group = where[0], where[1]
    rows = embed.shape[0]
    size = 6 * rows
    embed_whole[block(group, rows)] = embed[...]
    for source, core in ((mine, 0), (others, 1)):
        for n in range(SPREAD // 2):
            p = piece ^ (2 * n + core)
            for k in range(3):
                at = n * size + k * rows
                embed_whole[block(group ^ (k + 1), rows), lanes(p)] = source[at : at + rows]
                at += 3 * rows
                attn_far[attn_unit(attn_far, 3 * p + k)] = source[at : at + rows]


def place_mlp_kernel(where, mine, others, up_far, down_far):
    piece = where[0]
    size = up_far.shape[0] // SPREAD
    for source, core in ((mine, 0), (others, 1)):
        for n in range(SPREAD // 2):
            p = piece ^ (2 * n + core)
            at = n * 2 * size
            up_far[block(p, size)] = source[at : at + size]
            down_far[block(p, size)] = source[at + size : at + 2 * size]


def neighbours_of(where, piece):
    parts = [piece]
    for bits in range(2, SPREAD, 2):
        parts.append(swap(piece, "dp", bits))
    rows = len(parts) * piece.shape[0]
    mine = copier(stack_kernel, ((rows,) + piece.shape[1:],), where, *parts)[0]
    return mine, swap(mine, "dp", 1)


def turned_dot(left, right):
    return lax.dot_general(left, right, (((1,), (1,)), ((), ())), preferred_element_type=F32)


def columns_dot(left, right):
    return lax.dot_general(left, right, (((0,), (0,)), ((), ())), preferred_element_type=F32)


def context_of(normed, shard):
    width = shard.shape[0] // 4
    projected = turned_dot(shard[: 3 * width], normed).astype(BF16)
    results = []
    for at in range(0, width, HEAD_DIM):
        queries, attn_keys, attn_values = (
            projected[c * width + at : c * width + at + HEAD_DIM] for c in range(3)
        )
        scores = columns_dot(attn_keys, queries) * HEAD_DIM ** (-0.5)
        raised = jnp.exp(scores - jnp.max(scores, axis=0, keepdims=True))
        probs = (raised / jnp.sum(raised, axis=0, keepdims=True)).astype(BF16)
        results.append(dot(attn_values, probs).astype(BF16))
    return results


def attend_kernel(where, kept, opposite, neighbour, third, embed, own, far, gain, mine, other):
    group = where[1]
    quarter, pixel_width = kept.shape
    count = embed.shape[1] - pixel_width
    pixels = jnp.concatenate([kept[...], opposite[...], neighbour[...], third[...]], axis=0)
    row = lax.broadcasted_iota(jnp.int32, (count, count), 0)
    column = lax.broadcasted_iota(jnp.int32, (count, count), 1)
    block_of = row // quarter
    turned = (block_of >> 1) + 2 * (block_of & 1)
    spot = (turned ^ group) * quarter + row % quarter
    picks = jnp.where(spot == column, 1.0, 0.0).astype(BF16)
    product = turned_dot(pixels, embed[:, :pixel_width]) + turned_dot(picks, embed[:, pixel_width:])
    activations = product.astype(BF16).astype(F32)
    normed = norm_rows(activations, gain[...]).astype(BF16)
    width = own.shape[0] // 4
    context = jnp.concatenate(context_of(normed, own) + context_of(normed, far), axis=0)
    out = jnp.concatenate([own[3 * width :], far[3 * width :]], axis=0)
    attended = columns_dot(context, out)
    half = 2 * quarter
    mine[...] = activations[:half] + attended[:half]
    other[...] = attended[half:].astype(BF16)


def attend(where, parts, embed, own, far, gain):
    half = 2 * parts[0].shape[0]
    model = own.shape[1]
    held = [pltpu.with_memory_space_constraint(x, pltpu.VMEM) for x in (*parts, embed, own, far)]
    return pl.pallas_call(
        attend_kernel,
        in_specs=[SCALARS] + [FAST] * 8,
        out_specs=(FAST, FAST),
        out_shape=(pltpu.VMEM((half, model), F32), pltpu.VMEM((half, model), BF16)),
        compiler_params=pltpu.CompilerParams(vmem_limit_bytes=20 * 1024 * 1024),
    )(where, *held, gain.reshape(1, -1))


def gelu(values):
    return 0.5 * values * (1.0 + lax.erf(values * 0.5 ** 0.5))


def feed_through(normed, up, down):
    return dot(gelu(dot(normed, up)).astype(BF16), down)


def first_kernel(normed, up_far, down_far, up, down, feed, up_own, down_own, sem):
    copies = [
        pltpu.make_async_copy(up, up_own, sem.at[0]),
        pltpu.make_async_copy(down, down_own, sem.at[1]),
    ]
    for copy in copies:
        copy.start()
    part = feed_through(normed[...], up_far[...], down_far[...])
    for copy in copies:
        copy.wait()
    feed[...] = part + feed_through(normed[...], up_own[...], down_own[...])


def feed_first(normed, up_far, down_far, up, down):
    held = [pltpu.with_memory_space_constraint(x, pltpu.VMEM) for x in (normed, up_far, down_far)]
    return pl.pallas_call(
        first_kernel,
        in_specs=[FAST, FAST, FAST, SLOW, SLOW],
        out_specs=(FAST, FAST, FAST),
        out_shape=(
            pltpu.VMEM((normed.shape[0], down.shape[1]), F32),
            pltpu.VMEM(up.shape, BF16),
            pltpu.VMEM(down.shape, BF16),
        ),
        scratch_shapes=[pltpu.SemaphoreType.DMA((2,))],
        compiler_params=pltpu.CompilerParams(vmem_limit_bytes=16 * 1024 * 1024),
    )(*held, *(pltpu.with_memory_space_constraint(x, pltpu.HBM) for x in (up, down)))


def second_kernel(normed, up_far, down_far, up_own, down_own, near, third):
    part = feed_through(normed[...], up_far[...], down_far[...])
    part = part + feed_through(normed[...], up_own[...], down_own[...])
    quarter = near.shape[0]
    near[...] = part[:quarter].astype(BF16)
    third[...] = part[quarter:].astype(BF16)


def feed_second(*operands):
    half, model = operands[0].shape
    held = [pltpu.with_memory_space_constraint(x, pltpu.VMEM) for x in operands]
    return pl.pallas_call(
        second_kernel,
        in_specs=[FAST] * 5,
        out_specs=(FAST, FAST),
        out_shape=(pltpu.VMEM((half // 2, model), BF16), pltpu.VMEM((half // 2, model), BF16)),
        compiler_params=pltpu.CompilerParams(vmem_limit_bytes=16 * 1024 * 1024),
    )(*held)


def layer(
    candidates,
    owner_row,
    selected,
    dest_slot,
    patch_weight,
    positions,
    qkv_weight,
    out_weight,
    attn_gain,
    mlp_gain,
    up_weight,
    down_weight,
):
    groups = lax.axis_size("mp")
    group = lax.axis_index("mp")
    pair = group // 2
    quarter = candidates.shape[1]
    where = jnp.stack([lax.axis_index("dp") % SPREAD, group]).astype(jnp.int32)

    outgoing, senders = route(owner_row, selected, dest_slot, candidates)
    incoming = lax.all_to_all(outgoing, "dp", split_axis=0, concat_axis=0, tiled=True)

    pixel_width, width = patch_weight.shape
    model = out_weight.shape[1]
    embed_own = jnp.concatenate([patch_weight.T, positions.T], axis=1)
    attn_own = jnp.concatenate([qkv_weight.transpose(1, 2, 0).reshape(-1, model), out_weight])
    embed_piece, both_piece, mlp_piece = extract(where, embed_own, attn_own, up_weight, down_weight)
    third = swap(embed_piece, "mp", 3)
    opposite = swap(both_piece, "mp", 2)
    neighbour = swap(embed_piece, "mp", 1)
    units = copier(units_kernel, ((6 * width, UNIT),), where, neighbour, opposite, third)[0]
    embed_whole, attn_far = copier(
        place_attn_kernel,
        ((groups * width, pixel_width + positions.shape[0]), attn_own.shape),
        where,
        embed_own,
        *neighbours_of(where, units),
    )
    mlp_piece = swap(mlp_piece, "mp", 2)
    up_far, down_far = copier(
        place_mlp_kernel,
        (up_weight.shape, down_weight.shape),
        where,
        *neighbours_of(where, mlp_piece),
    )

    kept, given = choose(where, senders, incoming)
    third = swap(given, "mp", 3)
    opposite = swap(given, "mp", 2)
    neighbour = swap(kept, "mp", 1)
    mine, other = attend(
        where, (kept, opposite, neighbour, third), embed_whole, attn_own, attn_far, attn_gain
    )
    other = swap(other, "mp", 1)
    after_attn = mine + other.astype(F32)
    gain2 = widen(mlp_gain)
    normed2 = norm_rows(after_attn, gain2).astype(BF16)
    neighbour2 = swap(normed2, "mp", 1)
    feed, up_own, down_own = feed_first(normed2, up_far, down_far, up_weight, down_weight)
    from_opposite = swap((after_attn + feed)[quarter:].astype(BF16), "mp", 2)
    for_near, for_third = feed_second(neighbour2, up_far, down_far, up_own, down_own)
    from_third = swap(for_third, "mp", 3)
    from_neighbour = swap(for_near, "mp", 1)
    kept_out = (after_attn[:quarter] + (feed[:quarter] + from_neighbour.astype(F32))).astype(BF16)
    given_out = (from_opposite.astype(F32) + from_third.astype(F32)).astype(BF16)
    swapped = pair == 1
    return jnp.stack(
        [jnp.where(swapped, given_out, kept_out), jnp.where(swapped, kept_out, given_out)]
    )


def solution(mesh):
    return jax.shard_map(
        layer,
        mesh=mesh,
        in_specs=(
            P("dp", "mp", None),
            P(),
            P(),
            P(),
            P(None, "mp"),
            P(None, "mp"),
            P(None, None, "mp"),
            P("mp", None),
            P(),
            P(),
            P(None, "mp"),
            P("mp", None),
        ),
        out_specs=P("dp", "mp", None),
        check_vma=False,
    )
```

```python
import jax
import jax.numpy as jnp
from jax import lax
from jax.experimental import pallas as pl
from jax.experimental.pallas import tpu as pltpu
from jax.sharding import PartitionSpec as P

CAND_DEV = 8
SEL_DEV = 2
HEAD_DIM = 64
SPREAD = 8
BF16 = jnp.bfloat16
F32 = jnp.float32


def norm_rows(values, gain):
    average = jnp.mean(values, axis=-1, keepdims=True)
    centred = values - average
    variance = jnp.mean(centred * centred, axis=-1, keepdims=True)
    return centred * lax.rsqrt(variance + 1e-06) * gain.astype(F32)


def swap(value, axis, bits):
    return lax.ppermute(value, axis, [(i, i ^ bits) for i in range(lax.axis_size(axis))])


def dot(left, right):
    return jnp.dot(left, right, preferred_element_type=F32)


ANY = pl.BlockSpec(memory_space=pl.ANY)
SCALARS = pl.BlockSpec(memory_space=pltpu.SMEM)
FAST = pl.BlockSpec(memory_space=pltpu.VMEM)
SLOW = pl.BlockSpec(memory_space=pltpu.HBM)
UNIT = 128
SMALL = pltpu.CompilerParams(vmem_limit_bytes=4 * 1024 * 1024)


def copier(body, outs, where, *operands):
    return pl.pallas_call(
        body,
        in_specs=[SCALARS] + [FAST] * len(operands),
        out_specs=tuple(FAST for _ in outs),
        out_shape=tuple(pltpu.VMEM(shape, BF16) for shape in outs),
        compiler_params=SMALL,
    )(where, *(pltpu.with_memory_space_constraint(x, pltpu.VMEM) for x in operands))


def route_kernel(own, owner_row, selected, dest_slot, candidates, outgoing, senders, sem):
    me = own[0]

    def visit(i, sent):
        row = owner_row[selected[i]]
        owner = row // CAND_DEV
        slot = dest_slot[i]

        @pl.when(slot // SEL_DEV == me)
        def _():
            senders[slot % SEL_DEV] = owner

        @pl.when(owner == me)
        def _():
            pltpu.make_async_copy(
                candidates.at[row % CAND_DEV], outgoing.at[slot // SEL_DEV], sem.at[0]
            ).start()

        return sent + (owner == me).astype(jnp.int32)

    sent = lax.fori_loop(0, selected.shape[0], visit, 0)

    def finish(_, carry):
        pltpu.make_async_copy(candidates.at[0], outgoing.at[0], sem.at[0]).wait()
        return carry

    lax.fori_loop(0, sent, finish, 0)


def route(owner_row, selected, dest_slot, candidates):
    learners = lax.axis_size("dp")
    own = jnp.full((1,), lax.axis_index("dp"), jnp.int32)
    shape = (learners,) + candidates.shape[1:]
    small = learners <= 2 * SPREAD
    return pl.pallas_call(
        route_kernel,
        in_specs=[SCALARS] * 4 + [ANY],
        out_specs=(FAST, SCALARS),
        out_shape=(
            pltpu.VMEM(shape, BF16) if small else jax.ShapeDtypeStruct(shape, BF16),
            jax.ShapeDtypeStruct((SEL_DEV,), jnp.int32),
        ),
        scratch_shapes=[pltpu.SemaphoreType.DMA((1,))],
        compiler_params=pltpu.CompilerParams(vmem_limit_bytes=24 * 1024 * 1024),
    )(own, owner_row, selected, dest_slot, candidates)


def choose_kernel(where, senders, incoming, kept, given, sem):
    pair = where[1] // 2
    copies = [
        pltpu.make_async_copy(incoming.at[senders[pair]], kept, sem.at[0]),
        pltpu.make_async_copy(incoming.at[senders[1 - pair]], given, sem.at[1]),
    ]
    for copy in copies:
        copy.start()
    for copy in copies:
        copy.wait()


def choose(where, senders, incoming):
    shape = incoming.shape[1:]
    return pl.pallas_call(
        choose_kernel,
        in_specs=[SCALARS, SCALARS, SLOW],
        out_specs=(FAST, FAST),
        out_shape=(pltpu.VMEM(shape, BF16), pltpu.VMEM(shape, BF16)),
        scratch_shapes=[pltpu.SemaphoreType.DMA((2,))],
        compiler_params=SMALL,
    )(where, senders, pltpu.with_memory_space_constraint(incoming, pltpu.HBM))


def widen_kernel(values, wide):
    wide[...] = values[...].astype(F32)


def widen(values):
    row = values.reshape(1, -1)
    return pl.pallas_call(
        widen_kernel,
        in_specs=[FAST],
        out_specs=FAST,
        out_shape=jax.ShapeDtypeStruct(row.shape, F32),
        compiler_params=SMALL,
    )(row)


def attn_unit(array, unit):
    columns = array.shape[1] // UNIT
    rows = array.shape[0] // 4
    return (
        pl.ds(pl.multiple_of((unit // columns) * rows, rows), rows),
        pl.ds(pl.multiple_of((unit % columns) * UNIT, UNIT), UNIT),
    )


def lanes(index):
    return pl.ds(pl.multiple_of(index * UNIT, UNIT), UNIT)


def block(index, size):
    return pl.ds(pl.multiple_of(index * size, size), size)


def extract_kernel(where, embed, attn, up, down, embed_piece, both_piece, mlp_piece, sem):
    piece = where[0]
    rows = embed.shape[0]
    size = up.shape[0] // SPREAD
    copies = [
        pltpu.make_async_copy(up.at[block(piece, size)], mlp_piece.at[pl.ds(0, size)], sem.at[0]),
        pltpu.make_async_copy(
            down.at[block(piece, size)], mlp_piece.at[pl.ds(size, size)], sem.at[1]
        ),
    ]
    for copy in copies:
        copy.start()
    unit = embed[:, lanes(piece)]
    embed_piece[...] = unit
    both_piece[:rows] = unit
    for i in range(3):
        both_piece[(1 + i) * rows : (2 + i) * rows] = attn[attn_unit(attn, 3 * piece + i)]
    for copy in copies:
        copy.wait()


def extract(where, embed, attn, up, down):
    rows = embed.shape[0]
    return pl.pallas_call(
        extract_kernel,
        in_specs=[SCALARS, FAST, FAST, SLOW, SLOW],
        out_specs=(FAST, FAST, FAST),
        out_shape=(
            pltpu.VMEM((rows, UNIT), BF16),
            pltpu.VMEM((4 * rows, UNIT), BF16),
            pltpu.VMEM((2 * up.shape[0] // SPREAD, up.shape[1]), BF16),
        ),
        scratch_shapes=[pltpu.SemaphoreType.DMA((2,))],
        compiler_params=SMALL,
    )(
        where,
        pltpu.with_memory_space_constraint(embed, pltpu.VMEM),
        pltpu.with_memory_space_constraint(attn, pltpu.VMEM),
        pltpu.with_memory_space_constraint(up, pltpu.HBM),
        pltpu.with_memory_space_constraint(down, pltpu.HBM),
    )


def units_kernel(where, neighbour, opposite, third, target):
    rows = neighbour.shape[0]
    target[:rows] = neighbour[...]
    target[rows : 2 * rows] = opposite[:rows]
    target[2 * rows : 3 * rows] = third[...]
    target[3 * rows :] = opposite[rows:]


def stack_kernel(where, *refs):
    *parts, target = refs
    rows = parts[0].shape[0]
    for n, part in enumerate(parts):
        target[n * rows : (n + 1) * rows] = part[...]


def place_attn_kernel(where, embed, *refs):
    *pieces, embed_whole, attn_far = refs
    piece, group = where[0], where[1]
    rows = embed.shape[0]
    embed_whole[block(group, rows)] = embed[...]
    for n, source in enumerate(pieces):
        p = piece ^ (2 * (n % (SPREAD // 2)) + n // (SPREAD // 2))
        for k in range(3):
            at = k * rows
            embed_whole[block(group ^ (k + 1), rows), lanes(p)] = source[at : at + rows]
            at += 3 * rows
            attn_far[attn_unit(attn_far, 3 * p + k)] = source[at : at + rows]


def place_mlp_kernel(where, mine, others, up_far, down_far):
    piece = where[0]
    size = up_far.shape[0] // SPREAD
    for source, core in ((mine, 0), (others, 1)):
        for n in range(SPREAD // 2):
            p = piece ^ (2 * n + core)
            at = n * 2 * size
            up_far[block(p, size)] = source[at : at + size]
            down_far[block(p, size)] = source[at + size : at + 2 * size]


def neighbours_of(piece):
    parts = [piece]
    for bits in range(2, SPREAD, 2):
        parts.append(swap(piece, "dp", bits))
    return parts


def other_core(value):
    return swap(value, "dp", 1)


def turned_dot(left, right):
    return lax.dot_general(left, right, (((1,), (1,)), ((), ())), preferred_element_type=F32)


def columns_dot(left, right):
    return lax.dot_general(left, right, (((0,), (0,)), ((), ())), preferred_element_type=F32)


def attended_of(projected, shards, start, stop):
    results = []
    for values, shard in zip(projected, shards):
        width = shard.shape[0] // 4
        for at in range(0, width, HEAD_DIM):
            queries, attn_keys, attn_values = (
                values[c * width + at : c * width + at + HEAD_DIM] for c in range(3)
            )
            scores = columns_dot(attn_keys, queries[:, start:stop]) * HEAD_DIM ** (-0.5)
            raised = jnp.exp(scores - jnp.max(scores, axis=0, keepdims=True))
            probs = (raised / jnp.sum(raised, axis=0, keepdims=True)).astype(BF16)
            results.append(dot(attn_values, probs).astype(BF16))
    out = jnp.concatenate([shard[3 * (shard.shape[0] // 4) :] for shard in shards], axis=0)
    return columns_dot(jnp.concatenate(results, axis=0), out)


def attend_kernel(
    where, kept, opposite, neighbour, third, embed, own, far, gain, own_qkv, far_qkv, embedded, other
):
    group = where[1]
    quarter, pixel_width = kept.shape
    count = embed.shape[1] - pixel_width
    half = 2 * quarter
    pixels = jnp.concatenate([kept[...], opposite[...], neighbour[...], third[...]], axis=0)
    row = lax.broadcasted_iota(jnp.int32, (count, count), 0)
    column = lax.broadcasted_iota(jnp.int32, (count, count), 1)
    block_of = row // quarter
    turned = (block_of >> 1) + 2 * (block_of & 1)
    spot = (turned ^ group) * quarter + row % quarter
    picks = jnp.where(spot == column, 1.0, 0.0).astype(BF16)
    product = turned_dot(pixels, embed[:, :pixel_width]) + turned_dot(picks, embed[:, pixel_width:])
    rounded = product.astype(BF16)
    embedded[...] = rounded[:half]
    normed = norm_rows(rounded.astype(F32), gain[...]).astype(BF16)
    width = own.shape[0] // 4
    projected = [turned_dot(shard[: 3 * width], normed).astype(BF16) for shard in (own, far)]
    own_qkv[...] = projected[0]
    far_qkv[...] = projected[1]
    other[...] = attended_of(projected, (own, far), half, count).astype(BF16)


def attend_mine_kernel(own_qkv, far_qkv, embedded, own, far, up, down, mine, up_own, down_own, sem):
    copies = [
        pltpu.make_async_copy(up, up_own, sem.at[0]),
        pltpu.make_async_copy(down, down_own, sem.at[1]),
    ]
    for copy in copies:
        copy.start()
    projected = (own_qkv[...], far_qkv[...])
    half = embedded.shape[0]
    mine[...] = embedded[...].astype(F32) + attended_of(projected, (own, far), 0, half)
    for copy in copies:
        copy.wait()


def held(operands):
    return [pltpu.with_memory_space_constraint(x, pltpu.VMEM) for x in operands]


def attend(where, parts, embed, own, far, gain):
    half = 2 * parts[0].shape[0]
    rows, model = own.shape
    qkv = (rows // 4 * 3, 2 * half)
    return pl.pallas_call(
        attend_kernel,
        in_specs=[SCALARS] + [FAST] * 8,
        out_specs=(FAST,) * 4,
        out_shape=tuple(
            pltpu.VMEM(shape, BF16) for shape in (qkv, qkv, (half, model), (half, model))
        ),
        compiler_params=pltpu.CompilerParams(vmem_limit_bytes=20 * 1024 * 1024),
    )(where, *held((*parts, embed, own, far)), gain.reshape(1, -1))


def attend_mine(embedded, own_qkv, far_qkv, own, far, up, down):
    return pl.pallas_call(
        attend_mine_kernel,
        in_specs=[FAST] * 5 + [SLOW] * 2,
        out_specs=(FAST,) * 3,
        out_shape=(
            pltpu.VMEM(embedded.shape, F32),
            pltpu.VMEM(up.shape, BF16),
            pltpu.VMEM(down.shape, BF16),
        ),
        scratch_shapes=[pltpu.SemaphoreType.DMA((2,))],
        compiler_params=pltpu.CompilerParams(vmem_limit_bytes=12 * 1024 * 1024),
    )(
        *held((own_qkv, far_qkv, embedded, own, far)),
        *(pltpu.with_memory_space_constraint(x, pltpu.HBM) for x in (up, down)),
    )


def join_kernel(mine, other, gain, after_attn, normed2):
    after = mine[...] + other[...].astype(F32)
    after_attn[...] = after
    normed2[...] = norm_rows(after, gain[...]).astype(BF16)


def join(mine, other, gain):
    return pl.pallas_call(
        join_kernel,
        in_specs=[FAST] * 3,
        out_specs=(FAST, FAST),
        out_shape=(pltpu.VMEM(mine.shape, F32), pltpu.VMEM(mine.shape, BF16)),
        compiler_params=SMALL,
    )(*held((mine, other)), gain)


def gelu(values):
    return 0.5 * values * (1.0 + lax.erf(values * 0.5 ** 0.5))


def feed_through(normed, up, down):
    return dot(gelu(dot(normed, up)).astype(BF16), down)


def own_kernel(normed, up, down, feed):
    feed[...] = feed_through(normed[...], up[...], down[...])


def first_kernel(normed, up, down, part, feed):
    feed[...] = part[...] + feed_through(normed[...], up[...], down[...])


def feed_first(body, *operands):
    return pl.pallas_call(
        body,
        in_specs=[FAST] * len(operands),
        out_specs=FAST,
        out_shape=pltpu.VMEM(operands[0].shape, F32),
        compiler_params=pltpu.CompilerParams(vmem_limit_bytes=16 * 1024 * 1024),
    )(*held(operands))


def second_kernel(normed, up_far, down_far, up_own, down_own, near, third):
    part = feed_through(normed[...], up_far[...], down_far[...])
    part = part + feed_through(normed[...], up_own[...], down_own[...])
    quarter = near.shape[0]
    near[...] = part[:quarter].astype(BF16)
    third[...] = part[quarter:].astype(BF16)


def feed_second(*operands):
    half, model = operands[0].shape
    return pl.pallas_call(
        second_kernel,
        in_specs=[FAST] * 5,
        out_specs=(FAST, FAST),
        out_shape=(pltpu.VMEM((half // 2, model), BF16), pltpu.VMEM((half // 2, model), BF16)),
        compiler_params=pltpu.CompilerParams(vmem_limit_bytes=16 * 1024 * 1024),
    )(*held(operands))


def layer(
    candidates,
    owner_row,
    selected,
    dest_slot,
    patch_weight,
    positions,
    qkv_weight,
    out_weight,
    attn_gain,
    mlp_gain,
    up_weight,
    down_weight,
):
    groups = lax.axis_size("mp")
    group = lax.axis_index("mp")
    pair = group // 2
    quarter = candidates.shape[1]
    where = jnp.stack([lax.axis_index("dp") % SPREAD, group]).astype(jnp.int32)

    outgoing, senders = route(owner_row, selected, dest_slot, candidates)
    incoming = lax.all_to_all(outgoing, "dp", split_axis=0, concat_axis=0, tiled=True)

    pixel_width, width = patch_weight.shape
    model = out_weight.shape[1]
    embed_own = jnp.concatenate([patch_weight.T, positions.T], axis=1)
    attn_own = jnp.concatenate([qkv_weight.transpose(1, 2, 0).reshape(-1, model), out_weight])
    embed_piece, both_piece, mlp_piece = extract(where, embed_own, attn_own, up_weight, down_weight)
    third = swap(embed_piece, "mp", 3)
    opposite = swap(both_piece, "mp", 2)
    neighbour = swap(embed_piece, "mp", 1)
    units = copier(units_kernel, ((6 * width, UNIT),), where, neighbour, opposite, third)[0]
    near = neighbours_of(units)
    far = [other_core(part) for part in near]
    embed_whole, attn_far = copier(
        place_attn_kernel,
        ((groups * width, pixel_width + positions.shape[0]), attn_own.shape),
        where,
        embed_own,
        *near,
        *far,
    )
    mlp_piece = swap(mlp_piece, "mp", 2)
    near2 = neighbours_of(mlp_piece)
    rows2 = len(near2) * mlp_piece.shape[0]
    mine2 = copier(stack_kernel, ((rows2, model),), where, *near2)[0]
    far2 = other_core(mine2)
    up_far, down_far = copier(
        place_mlp_kernel, (up_weight.shape, down_weight.shape), where, mine2, far2
    )

    kept, given = choose(where, senders, incoming)
    third = swap(given, "mp", 3)
    opposite = swap(given, "mp", 2)
    neighbour = swap(kept, "mp", 1)
    own_qkv, far_qkv, embedded, other = attend(
        where, (kept, opposite, neighbour, third), embed_whole, attn_own, attn_far, attn_gain
    )
    other = swap(other, "mp", 1)
    mine, up_own, down_own = attend_mine(
        embedded, own_qkv, far_qkv, attn_own, attn_far, up_weight, down_weight
    )
    gain2 = widen(mlp_gain)
    after_attn, normed2 = join(mine, other, gain2)
    neighbour2 = swap(normed2, "mp", 1)
    feed = feed_first(own_kernel, normed2, up_own, down_own)
    feed = feed_first(first_kernel, normed2, up_far, down_far, feed)
    from_opposite = swap((after_attn + feed)[quarter:].astype(BF16), "mp", 2)
    for_near, for_third = feed_second(neighbour2, up_far, down_far, up_own, down_own)
    from_third = swap(for_third, "mp", 3)
    from_neighbour = swap(for_near, "mp", 1)
    kept_out = (after_attn[:quarter] + (feed[:quarter] + from_neighbour.astype(F32))).astype(BF16)
    given_out = (from_opposite.astype(F32) + from_third.astype(F32)).astype(BF16)
    swapped = pair == 1
    return jnp.stack(
        [jnp.where(swapped, given_out, kept_out), jnp.where(swapped, kept_out, given_out)]
    )


def solution(mesh):
    return jax.shard_map(
        layer,
        mesh=mesh,
        in_specs=(
            P("dp", "mp", None),
            P(),
            P(),
            P(),
            P(None, "mp"),
            P(None, "mp"),
            P(None, None, "mp"),
            P("mp", None),
            P(),
            P(),
            P(None, "mp"),
            P("mp", None),
        ),
        out_specs=P("dp", "mp", None),
        check_vma=False,
    )
```

```python
import jax
import jax.numpy as jnp
from jax import lax
from jax.experimental import pallas as pl
from jax.experimental.pallas import tpu as pltpu
from jax.sharding import PartitionSpec as P

CAND_DEV = 8
SEL_DEV = 2
HEAD_DIM = 64
SPREAD = 8
CHIPS = (0, 6, 2, 4)
BF16 = jnp.bfloat16
F32 = jnp.float32


def norm_rows(values, gain):
    average = jnp.mean(values, axis=-1, keepdims=True)
    centred = values - average
    variance = jnp.mean(centred * centred, axis=-1, keepdims=True)
    return centred * lax.rsqrt(variance + 1e-06) * gain.astype(F32)


def swap(value, axis, bits):
    return lax.ppermute(value, axis, [(i, i ^ bits) for i in range(lax.axis_size(axis))])


def dot(left, right):
    return jnp.dot(left, right, preferred_element_type=F32)


ANY = pl.BlockSpec(memory_space=pl.ANY)
SCALARS = pl.BlockSpec(memory_space=pltpu.SMEM)
FAST = pl.BlockSpec(memory_space=pltpu.VMEM)
SLOW = pl.BlockSpec(memory_space=pltpu.HBM)
UNIT = 128
SMALL = pltpu.CompilerParams(vmem_limit_bytes=4 * 1024 * 1024)


def copier(body, outs, where, *operands, aliases={}):
    return pl.pallas_call(
        body,
        in_specs=[SCALARS] + [FAST] * len(operands),
        out_specs=tuple(FAST for _ in outs),
        out_shape=tuple(pltpu.VMEM(shape, BF16) for shape in outs),
        compiler_params=SMALL,
        input_output_aliases=aliases,
    )(where, *(pltpu.with_memory_space_constraint(x, pltpu.VMEM) for x in operands))


def route_kernel(
    own, owner_row, selected, dest_slot, candidates, up, down, outgoing, senders, mlp_piece, sem
):
    me = own[0]
    size = up.shape[0] // SPREAD
    copies = [
        pltpu.make_async_copy(
            source.at[block(me % SPREAD, size)], mlp_piece.at[pl.ds(n * size, size)], sem.at[1 + n]
        )
        for n, source in enumerate((up, down))
    ]
    for copy in copies:
        copy.start()

    def visit(i, sent):
        row = owner_row[selected[i]]
        owner = row // CAND_DEV
        slot = dest_slot[i]

        @pl.when(slot // SEL_DEV == me)
        def _():
            senders[slot % SEL_DEV] = owner

        @pl.when(owner == me)
        def _():
            pltpu.make_async_copy(
                candidates.at[row % CAND_DEV], outgoing.at[slot // SEL_DEV], sem.at[0]
            ).start()

        return sent + (owner == me).astype(jnp.int32)

    sent = lax.fori_loop(0, selected.shape[0], visit, 0)

    def finish(_, carry):
        pltpu.make_async_copy(candidates.at[0], outgoing.at[0], sem.at[0]).wait()
        return carry

    lax.fori_loop(0, sent, finish, 0)
    for copy in copies:
        copy.wait()


def route(owner_row, selected, dest_slot, candidates, up, down):
    learners = lax.axis_size("dp")
    own = jnp.full((1,), lax.axis_index("dp"), jnp.int32)
    shape = (learners,) + candidates.shape[1:]
    small = learners <= 2 * SPREAD
    return pl.pallas_call(
        route_kernel,
        in_specs=[SCALARS] * 4 + [ANY, SLOW, SLOW],
        out_specs=(FAST, SCALARS, FAST),
        out_shape=(
            pltpu.VMEM(shape, BF16) if small else jax.ShapeDtypeStruct(shape, BF16),
            jax.ShapeDtypeStruct((SEL_DEV,), jnp.int32),
            pltpu.VMEM((2 * up.shape[0] // SPREAD, up.shape[1]), BF16),
        ),
        scratch_shapes=[pltpu.SemaphoreType.DMA((3,))],
        compiler_params=pltpu.CompilerParams(vmem_limit_bytes=24 * 1024 * 1024),
    )(
        own,
        owner_row,
        selected,
        dest_slot,
        candidates,
        *(pltpu.with_memory_space_constraint(x, pltpu.HBM) for x in (up, down)),
    )


def choose_kernel(where, senders, incoming, kept, given, sem):
    pair = where[1] // 2
    copies = [
        pltpu.make_async_copy(incoming.at[senders[pair]], kept, sem.at[0]),
        pltpu.make_async_copy(incoming.at[senders[1 - pair]], given, sem.at[1]),
    ]
    for copy in copies:
        copy.start()
    for copy in copies:
        copy.wait()


def choose(where, senders, incoming):
    shape = incoming.shape[1:]
    return pl.pallas_call(
        choose_kernel,
        in_specs=[SCALARS, SCALARS, SLOW],
        out_specs=(FAST, FAST),
        out_shape=(pltpu.VMEM(shape, BF16), pltpu.VMEM(shape, BF16)),
        scratch_shapes=[pltpu.SemaphoreType.DMA((2,))],
        compiler_params=SMALL,
    )(where, senders, pltpu.with_memory_space_constraint(incoming, pltpu.HBM))


def widen_kernel(values, wide):
    wide[...] = values[...].astype(F32)


def widen(values):
    row = values.reshape(1, -1)
    return pl.pallas_call(
        widen_kernel,
        in_specs=[FAST],
        out_specs=FAST,
        out_shape=jax.ShapeDtypeStruct(row.shape, F32),
        compiler_params=SMALL,
    )(row)


def attn_unit(array, unit):
    columns = array.shape[1] // UNIT
    rows = array.shape[0] // 4
    return (
        pl.ds(pl.multiple_of((unit // columns) * rows, rows), rows),
        pl.ds(pl.multiple_of((unit % columns) * UNIT, UNIT), UNIT),
    )


def lanes(index):
    return pl.ds(pl.multiple_of(index * UNIT, UNIT), UNIT)


def block(index, size):
    return pl.ds(pl.multiple_of(index * size, size), size)


def extract_kernel(where, embed, attn, embed_piece, both_piece):
    piece = where[0]
    rows = embed.shape[0]
    unit = embed[:, lanes(piece)]
    embed_piece[...] = unit
    both_piece[:rows] = unit
    for i in range(3):
        both_piece[(1 + i) * rows : (2 + i) * rows] = attn[attn_unit(attn, 3 * piece + i)]


def units_kernel(where, neighbour, opposite, third, target):
    rows = neighbour.shape[0]
    target[:rows] = neighbour[...]
    target[rows : 2 * rows] = opposite[:rows]
    target[2 * rows : 3 * rows] = third[...]
    target[3 * rows :] = opposite[rows:]


def stack_kernel(where, *refs):
    *parts, target = refs
    rows = parts[0].shape[0]
    for n, part in enumerate(parts):
        target[n * rows : (n + 1) * rows] = part[...]


def place_pieces(where, pieces, first, embed_whole, attn_far):
    piece, group = where[0], where[1]
    rows = pieces[0].shape[0] // 6
    for n, source in enumerate(pieces, first):
        p = piece ^ (CHIPS[n % len(CHIPS)] + n // len(CHIPS))
        for k in range(3):
            at = k * rows
            embed_whole[block(group ^ (k + 1), rows), lanes(p)] = source[at : at + rows]
            at += 3 * rows
            attn_far[attn_unit(attn_far, 3 * p + k)] = source[at : at + rows]


def place_attn_kernel(where, embed, *refs):
    *pieces, embed_whole, attn_far = refs
    embed_whole[block(where[1], embed.shape[0])] = embed[...]
    place_pieces(where, pieces, 0, embed_whole, attn_far)


def place_rest_kernel(where, embed_in, attn_in, *refs):
    *pieces, embed_whole, attn_far = refs
    place_pieces(where, pieces, 2 * len(CHIPS) - len(pieces), embed_whole, attn_far)


def place_mlp_kernel(where, mine, others, up_far, down_far):
    piece = where[0]
    size = up_far.shape[0] // SPREAD
    for source, core in ((mine, 0), (others, 1)):
        for n, bits in enumerate(CHIPS):
            p = piece ^ (bits + core)
            at = n * 2 * size
            up_far[block(p, size)] = source[at : at + size]
            down_far[block(p, size)] = source[at + size : at + 2 * size]


def neighbours_of(piece):
    parts = [piece]
    for bits in CHIPS[1:]:
        parts.append(swap(piece, "dp", bits))
    return parts


def other_core(value):
    return swap(value, "dp", 1)


def turned_dot(left, right):
    return lax.dot_general(left, right, (((1,), (1,)), ((), ())), preferred_element_type=F32)


def columns_dot(left, right):
    return lax.dot_general(left, right, (((0,), (0,)), ((), ())), preferred_element_type=F32)


def attended_of(projected, shards, start, stop):
    results = []
    for values, shard in zip(projected, shards):
        width = shard.shape[0] // 4
        for at in range(0, width, HEAD_DIM):
            queries, attn_keys, attn_values = (
                values[c * width + at : c * width + at + HEAD_DIM] for c in range(3)
            )
            scores = columns_dot(attn_keys, queries[:, start:stop]) * HEAD_DIM ** (-0.5)
            raised = jnp.exp(scores - jnp.max(scores, axis=0, keepdims=True))
            probs = (raised / jnp.sum(raised, axis=0, keepdims=True)).astype(BF16)
            results.append(dot(attn_values, probs).astype(BF16))
    out = jnp.concatenate([shard[3 * (shard.shape[0] // 4) :] for shard in shards], axis=0)
    return columns_dot(jnp.concatenate(results, axis=0), out)


def attend_kernel(
    where, kept, opposite, neighbour, third, embed, own, far, gain, own_qkv, far_qkv, embedded, other
):
    group = where[1]
    quarter, pixel_width = kept.shape
    count = embed.shape[1] - pixel_width
    half = 2 * quarter
    pixels = jnp.concatenate([kept[...], third[...], neighbour[...], opposite[...]], axis=0)
    row = lax.broadcasted_iota(jnp.int32, (count, count), 0)
    column = lax.broadcasted_iota(jnp.int32, (count, count), 1)
    block_of = row // quarter
    turned = (block_of >> 1) ^ (3 * (block_of & 1))
    spot = (turned ^ group) * quarter + row % quarter
    picks = jnp.where(spot == column, 1.0, 0.0).astype(BF16)
    product = turned_dot(pixels, embed[:, :pixel_width]) + turned_dot(picks, embed[:, pixel_width:])
    rounded = product.astype(BF16)
    embedded[...] = rounded[:half]
    normed = norm_rows(rounded.astype(F32), gain[...]).astype(BF16)
    width = own.shape[0] // 4
    projected = [turned_dot(shard[: 3 * width], normed).astype(BF16) for shard in (own, far)]
    own_qkv[...] = projected[0]
    far_qkv[...] = projected[1]
    other[...] = attended_of(projected, (own, far), half, count).astype(BF16)


def attend_mine_kernel(own_qkv, far_qkv, embedded, own, far, up, down, mine, up_own, down_own, sem):
    copies = [
        pltpu.make_async_copy(up, up_own, sem.at[0]),
        pltpu.make_async_copy(down, down_own, sem.at[1]),
    ]
    for copy in copies:
        copy.start()
    projected = (own_qkv[...], far_qkv[...])
    half = embedded.shape[0]
    mine[...] = embedded[...].astype(F32) + attended_of(projected, (own, far), 0, half)
    for copy in copies:
        copy.wait()


def held(operands):
    return [pltpu.with_memory_space_constraint(x, pltpu.VMEM) for x in operands]


def attend(where, parts, embed, own, far, gain):
    half = 2 * parts[0].shape[0]
    rows, model = own.shape
    qkv = (rows // 4 * 3, 2 * half)
    return pl.pallas_call(
        attend_kernel,
        in_specs=[SCALARS] + [FAST] * 8,
        out_specs=(FAST,) * 4,
        out_shape=tuple(
            pltpu.VMEM(shape, BF16) for shape in (qkv, qkv, (half, model), (half, model))
        ),
        compiler_params=pltpu.CompilerParams(vmem_limit_bytes=20 * 1024 * 1024),
    )(where, *held((*parts, embed, own, far)), gain.reshape(1, -1))


def attend_mine(embedded, own_qkv, far_qkv, own, far, up, down):
    return pl.pallas_call(
        attend_mine_kernel,
        in_specs=[FAST] * 5 + [SLOW] * 2,
        out_specs=(FAST,) * 3,
        out_shape=(
            pltpu.VMEM(embedded.shape, F32),
            pltpu.VMEM(up.shape, BF16),
            pltpu.VMEM(down.shape, BF16),
        ),
        scratch_shapes=[pltpu.SemaphoreType.DMA((2,))],
        compiler_params=pltpu.CompilerParams(vmem_limit_bytes=12 * 1024 * 1024),
    )(
        *held((own_qkv, far_qkv, embedded, own, far)),
        *(pltpu.with_memory_space_constraint(x, pltpu.HBM) for x in (up, down)),
    )


def join_kernel(mine, other, gain, after_attn, normed2):
    after = mine[...] + other[...].astype(F32)
    after_attn[...] = after
    normed2[...] = norm_rows(after, gain[...]).astype(BF16)


def join(mine, other, gain):
    return pl.pallas_call(
        join_kernel,
        in_specs=[FAST] * 3,
        out_specs=(FAST, FAST),
        out_shape=(pltpu.VMEM(mine.shape, F32), pltpu.VMEM(mine.shape, BF16)),
        compiler_params=SMALL,
    )(*held((mine, other)), gain)


def gelu(values):
    return 0.5 * values * (1.0 + lax.erf(values * 0.5 ** 0.5))


def feed_through(normed, up, down):
    return dot(gelu(dot(normed, up)).astype(BF16), down)


def own_kernel(normed, up, down, feed):
    feed[...] = feed_through(normed[...], up[...], down[...])


def first_kernel(normed, up, down, part, feed):
    feed[...] = part[...] + feed_through(normed[...], up[...], down[...])


def feed_first(body, *operands):
    return pl.pallas_call(
        body,
        in_specs=[FAST] * len(operands),
        out_specs=FAST,
        out_shape=pltpu.VMEM(operands[0].shape, F32),
        compiler_params=pltpu.CompilerParams(vmem_limit_bytes=16 * 1024 * 1024),
    )(*held(operands))


def second_kernel(normed, up_far, down_far, up_own, down_own, near, opposite):
    part = feed_through(normed[...], up_far[...], down_far[...])
    part = part + feed_through(normed[...], up_own[...], down_own[...])
    quarter = near.shape[0]
    near[...] = part[:quarter].astype(BF16)
    opposite[...] = part[quarter:].astype(BF16)


def feed_second(*operands):
    half, model = operands[0].shape
    return pl.pallas_call(
        second_kernel,
        in_specs=[FAST] * 5,
        out_specs=(FAST, FAST),
        out_shape=(pltpu.VMEM((half // 2, model), BF16), pltpu.VMEM((half // 2, model), BF16)),
        compiler_params=pltpu.CompilerParams(vmem_limit_bytes=16 * 1024 * 1024),
    )(*held(operands))


def layer(
    candidates,
    owner_row,
    selected,
    dest_slot,
    patch_weight,
    positions,
    qkv_weight,
    out_weight,
    attn_gain,
    mlp_gain,
    up_weight,
    down_weight,
):
    groups = lax.axis_size("mp")
    group = lax.axis_index("mp")
    pair = group // 2
    quarter = candidates.shape[1]
    where = jnp.stack([lax.axis_index("dp") % SPREAD, group]).astype(jnp.int32)

    outgoing, senders, mlp_piece = route(
        owner_row, selected, dest_slot, candidates, up_weight, down_weight
    )
    incoming = lax.all_to_all(outgoing, "dp", split_axis=0, concat_axis=0, tiled=True)

    pixel_width, width = patch_weight.shape
    model = out_weight.shape[1]
    embed_own = jnp.concatenate([patch_weight.T, positions.T], axis=1)
    attn_own = jnp.concatenate([qkv_weight.transpose(1, 2, 0).reshape(-1, model), out_weight])
    embed_piece, both_piece = copier(
        extract_kernel, ((width, UNIT), (4 * width, UNIT)), where, embed_own, attn_own
    )
    third = swap(embed_piece, "mp", 3)
    opposite = swap(both_piece, "mp", 2)
    neighbour = swap(embed_piece, "mp", 1)
    units = copier(units_kernel, ((6 * width, UNIT),), where, neighbour, opposite, third)[0]
    near = neighbours_of(units)
    far = [other_core(part) for part in near]
    shapes = ((groups * width, pixel_width + positions.shape[0]), attn_own.shape)
    placed = copier(place_attn_kernel, shapes, where, embed_own, *near, *far[:2])
    embed_whole, attn_far = copier(
        place_rest_kernel, shapes, where, *placed, *far[2:], aliases={1: 0, 2: 1}
    )
    mlp_piece = swap(mlp_piece, "mp", 2)
    near2 = neighbours_of(mlp_piece)
    rows2 = len(near2) * mlp_piece.shape[0]
    mine2 = copier(stack_kernel, ((rows2, model),), where, *near2)[0]
    far2 = other_core(mine2)
    up_far, down_far = copier(
        place_mlp_kernel, (up_weight.shape, down_weight.shape), where, mine2, far2
    )

    kept, given = choose(where, senders, incoming)
    third = swap(given, "mp", 3)
    opposite = swap(given, "mp", 2)
    neighbour = swap(kept, "mp", 1)
    own_qkv, far_qkv, embedded, other = attend(
        where, (kept, opposite, neighbour, third), embed_whole, attn_own, attn_far, attn_gain
    )
    other = swap(other, "mp", 1)
    mine, up_own, down_own = attend_mine(
        embedded, own_qkv, far_qkv, attn_own, attn_far, up_weight, down_weight
    )
    gain2 = widen(mlp_gain)
    after_attn, normed2 = join(mine, other, gain2)
    neighbour2 = swap(normed2, "mp", 1)
    feed = feed_first(own_kernel, normed2, up_own, down_own)
    feed = feed_first(first_kernel, normed2, up_far, down_far, feed)
    from_third = swap((after_attn + feed)[quarter:].astype(BF16), "mp", 3)
    for_near, for_opposite = feed_second(neighbour2, up_far, down_far, up_own, down_own)
    from_opposite = swap(for_opposite, "mp", 2)
    from_neighbour = swap(for_near, "mp", 1)
    kept_out = (after_attn[:quarter] + (feed[:quarter] + from_neighbour.astype(F32))).astype(BF16)
    given_out = (from_opposite.astype(F32) + from_third.astype(F32)).astype(BF16)
    swapped = pair == 1
    return jnp.stack(
        [jnp.where(swapped, given_out, kept_out), jnp.where(swapped, kept_out, given_out)]
    )


def solution(mesh):
    return jax.shard_map(
        layer,
        mesh=mesh,
        in_specs=(
            P("dp", "mp", None),
            P(),
            P(),
            P(),
            P(None, "mp"),
            P(None, "mp"),
            P(None, None, "mp"),
            P("mp", None),
            P(),
            P(),
            P(None, "mp"),
            P("mp", None),
        ),
        out_specs=P("dp", "mp", None),
        check_vma=False,
    )
```

```python
import jax
import jax.numpy as jnp
from jax import lax
from jax.experimental import pallas as pl
from jax.experimental.pallas import tpu as pltpu
from jax.sharding import PartitionSpec as P

CAND_DEV = 8
SEL_DEV = 2
HEAD_DIM = 64
SPREAD = 8
CHIPS = (0, 6, 2, 4)
BF16 = jnp.bfloat16
F32 = jnp.float32


def norm_rows(values, gain):
    average = jnp.mean(values, axis=-1, keepdims=True)
    centred = values - average
    variance = jnp.mean(centred * centred, axis=-1, keepdims=True)
    return centred * lax.rsqrt(variance + 1e-06) * gain.astype(F32)


def swap(value, axis, bits):
    return lax.ppermute(value, axis, [(i, i ^ bits) for i in range(lax.axis_size(axis))])


def dot(left, right):
    return jnp.dot(left, right, preferred_element_type=F32)


ANY = pl.BlockSpec(memory_space=pl.ANY)
SCALARS = pl.BlockSpec(memory_space=pltpu.SMEM)
FAST = pl.BlockSpec(memory_space=pltpu.VMEM)
SLOW = pl.BlockSpec(memory_space=pltpu.HBM)
UNIT = 128
SMALL = pltpu.CompilerParams(vmem_limit_bytes=4 * 1024 * 1024)


def copier(body, outs, where, *operands, aliases={}):
    return pl.pallas_call(
        body,
        in_specs=[SCALARS] + [FAST] * len(operands),
        out_specs=tuple(FAST for _ in outs),
        out_shape=tuple(pltpu.VMEM(shape, BF16) for shape in outs),
        compiler_params=SMALL,
        input_output_aliases=aliases,
    )(where, *(pltpu.with_memory_space_constraint(x, pltpu.VMEM) for x in operands))


def route_kernel(
    own, owner_row, selected, dest_slot, candidates, up, down, outgoing, senders, mlp_piece, sem
):
    me = own[0]
    size = up.shape[0] // SPREAD
    copies = [
        pltpu.make_async_copy(
            source.at[block(me % SPREAD, size)], mlp_piece.at[pl.ds(n * size, size)], sem.at[1 + n]
        )
        for n, source in enumerate((up, down))
    ]
    for copy in copies:
        copy.start()

    def visit(i, sent):
        row = owner_row[selected[i]]
        owner = row // CAND_DEV
        slot = dest_slot[i]

        @pl.when(slot // SEL_DEV == me)
        def _():
            senders[slot % SEL_DEV] = owner

        @pl.when(owner == me)
        def _():
            pltpu.make_async_copy(
                candidates.at[row % CAND_DEV], outgoing.at[slot // SEL_DEV], sem.at[0]
            ).start()

        return sent + (owner == me).astype(jnp.int32)

    sent = lax.fori_loop(0, selected.shape[0], visit, 0)

    def finish(_, carry):
        pltpu.make_async_copy(candidates.at[0], outgoing.at[0], sem.at[0]).wait()
        return carry

    lax.fori_loop(0, sent, finish, 0)
    for copy in copies:
        copy.wait()


def route(owner_row, selected, dest_slot, candidates, up, down):
    learners = lax.axis_size("dp")
    own = jnp.full((1,), lax.axis_index("dp"), jnp.int32)
    shape = (learners,) + candidates.shape[1:]
    small = learners <= 2 * SPREAD
    return pl.pallas_call(
        route_kernel,
        in_specs=[SCALARS] * 4 + [ANY, SLOW, SLOW],
        out_specs=(FAST, SCALARS, FAST),
        out_shape=(
            pltpu.VMEM(shape, BF16) if small else jax.ShapeDtypeStruct(shape, BF16),
            jax.ShapeDtypeStruct((SEL_DEV,), jnp.int32),
            pltpu.VMEM((2 * up.shape[0] // SPREAD, up.shape[1]), BF16),
        ),
        scratch_shapes=[pltpu.SemaphoreType.DMA((3,))],
        compiler_params=pltpu.CompilerParams(vmem_limit_bytes=24 * 1024 * 1024),
    )(
        own,
        owner_row,
        selected,
        dest_slot,
        candidates,
        *(pltpu.with_memory_space_constraint(x, pltpu.HBM) for x in (up, down)),
    )


def choose_kernel(where, senders, incoming, kept, given, sem):
    pair = where[1] // 2
    copies = [
        pltpu.make_async_copy(incoming.at[senders[pair]], kept, sem.at[0]),
        pltpu.make_async_copy(incoming.at[senders[1 - pair]], given, sem.at[1]),
    ]
    for copy in copies:
        copy.start()
    for copy in copies:
        copy.wait()


def choose(where, senders, incoming):
    shape = incoming.shape[1:]
    return pl.pallas_call(
        choose_kernel,
        in_specs=[SCALARS, SCALARS, SLOW],
        out_specs=(FAST, FAST),
        out_shape=(pltpu.VMEM(shape, BF16), pltpu.VMEM(shape, BF16)),
        scratch_shapes=[pltpu.SemaphoreType.DMA((2,))],
        compiler_params=SMALL,
    )(where, senders, pltpu.with_memory_space_constraint(incoming, pltpu.HBM))


def widen_kernel(values, wide):
    wide[...] = values[...].astype(F32)


def widen(values):
    row = values.reshape(1, -1)
    return pl.pallas_call(
        widen_kernel,
        in_specs=[FAST],
        out_specs=FAST,
        out_shape=jax.ShapeDtypeStruct(row.shape, F32),
        compiler_params=SMALL,
    )(row)


def attn_unit(array, unit):
    columns = array.shape[1] // UNIT
    rows = array.shape[0] // 4
    return (
        pl.ds(pl.multiple_of((unit // columns) * rows, rows), rows),
        pl.ds(pl.multiple_of((unit % columns) * UNIT, UNIT), UNIT),
    )


def lanes(index):
    return pl.ds(pl.multiple_of(index * UNIT, UNIT), UNIT)


def block(index, size):
    return pl.ds(pl.multiple_of(index * size, size), size)


def extract_kernel(where, embed, attn, embed_piece, both_piece):
    piece = where[0]
    rows = embed.shape[0]
    unit = embed[:, lanes(piece)]
    embed_piece[...] = unit
    both_piece[:rows] = unit
    for i in range(3):
        both_piece[(1 + i) * rows : (2 + i) * rows] = attn[attn_unit(attn, 3 * piece + i)]


def units_kernel(where, neighbour, opposite, third, target):
    rows = neighbour.shape[0]
    target[:rows] = neighbour[...]
    target[rows : 2 * rows] = opposite[:rows]
    target[2 * rows : 3 * rows] = third[...]
    target[3 * rows :] = opposite[rows:]


def stack_kernel(where, *refs):
    *parts, target = refs
    rows = parts[0].shape[0]
    for n, part in enumerate(parts):
        target[n * rows : (n + 1) * rows] = part[...]


def place_pieces(where, pieces, first, embed_whole, attn_far):
    piece, group = where[0], where[1]
    rows = pieces[0].shape[0] // 6
    for n, source in enumerate(pieces, first):
        p = piece ^ (CHIPS[n % len(CHIPS)] + n // len(CHIPS))
        for k in range(3):
            at = k * rows
            embed_whole[block(group ^ (k + 1), rows), lanes(p)] = source[at : at + rows]
            at += 3 * rows
            attn_far[attn_unit(attn_far, 3 * p + k)] = source[at : at + rows]


def place_attn_kernel(where, embed, *refs):
    *pieces, embed_whole, attn_far = refs
    embed_whole[block(where[1], embed.shape[0])] = embed[...]
    place_pieces(where, pieces, 0, embed_whole, attn_far)


def place_rest_kernel(where, embed_in, attn_in, *refs):
    *pieces, embed_whole, attn_far = refs
    place_pieces(where, pieces, 2 * len(CHIPS) - len(pieces), embed_whole, attn_far)


def place_mlp_kernel(where, mine, others, up_far, down_far):
    piece = where[0]
    size = up_far.shape[0] // SPREAD
    for source, core in ((mine, 0), (others, 1)):
        for n, bits in enumerate(CHIPS):
            p = piece ^ (bits + core)
            at = n * 2 * size
            up_far[block(p, size)] = source[at : at + size]
            down_far[block(p, size)] = source[at + size : at + 2 * size]


def neighbours_of(piece):
    parts = [piece]
    for bits in CHIPS[1:]:
        parts.append(swap(piece, "dp", bits))
    return parts


def other_core(value):
    return swap(value, "dp", 1)


def turned_dot(left, right):
    return lax.dot_general(left, right, (((1,), (1,)), ((), ())), preferred_element_type=F32)


def columns_dot(left, right):
    return lax.dot_general(left, right, (((0,), (0,)), ((), ())), preferred_element_type=F32)


def attended_of(projected, shards, start, stop):
    results = []
    for values, shard in zip(projected, shards):
        width = shard.shape[0] // 4
        for at in range(0, width, HEAD_DIM):
            queries, attn_keys, attn_values = (
                values[c * width + at : c * width + at + HEAD_DIM] for c in range(3)
            )
            scores = columns_dot(attn_keys, queries[:, start:stop])
            raised = jnp.exp((scores - jnp.max(scores, axis=0, keepdims=True)) * HEAD_DIM ** (-0.5))
            share = 1.0 / jnp.sum(raised, axis=0, keepdims=True)
            probs = (raised * share).astype(BF16)
            results.append(dot(attn_values, probs).astype(BF16))
    out = jnp.concatenate([shard[3 * (shard.shape[0] // 4) :] for shard in shards], axis=0)
    return columns_dot(jnp.concatenate(results, axis=0), out)


def attend_kernel(
    where, kept, opposite, neighbour, third, embed, own, far, gain, own_qkv, far_qkv, embedded, other
):
    group = where[1]
    quarter, pixel_width = kept.shape
    count = embed.shape[1] - pixel_width
    half = 2 * quarter
    pixels = jnp.concatenate([kept[...], third[...], neighbour[...], opposite[...]], axis=0)
    row = lax.broadcasted_iota(jnp.int32, (count, count), 0)
    column = lax.broadcasted_iota(jnp.int32, (count, count), 1)
    block_of = row // quarter
    turned = (block_of >> 1) ^ (3 * (block_of & 1))
    spot = (turned ^ group) * quarter + row % quarter
    picks = jnp.where(spot == column, 1.0, 0.0).astype(BF16)
    product = turned_dot(pixels, embed[:, :pixel_width]) + turned_dot(picks, embed[:, pixel_width:])
    rounded = product.astype(BF16)
    embedded[...] = rounded[:half]
    normed = norm_rows(rounded.astype(F32), gain[...]).astype(BF16)
    width = own.shape[0] // 4
    projected = [turned_dot(shard[: 3 * width], normed).astype(BF16) for shard in (own, far)]
    own_qkv[...] = projected[0]
    far_qkv[...] = projected[1]
    other[...] = attended_of(projected, (own, far), half, count).astype(BF16)


def attend_mine_kernel(own_qkv, far_qkv, embedded, own, far, up, down, mine, up_own, down_own, sem):
    copies = [
        pltpu.make_async_copy(up, up_own, sem.at[0]),
        pltpu.make_async_copy(down, down_own, sem.at[1]),
    ]
    for copy in copies:
        copy.start()
    projected = (own_qkv[...], far_qkv[...])
    half = embedded.shape[0]
    mine[...] = embedded[...].astype(F32) + attended_of(projected, (own, far), 0, half)
    for copy in copies:
        copy.wait()


def held(operands):
    return [pltpu.with_memory_space_constraint(x, pltpu.VMEM) for x in operands]


def attend(where, parts, embed, own, far, gain):
    half = 2 * parts[0].shape[0]
    rows, model = own.shape
    qkv = (rows // 4 * 3, 2 * half)
    return pl.pallas_call(
        attend_kernel,
        in_specs=[SCALARS] + [FAST] * 8,
        out_specs=(FAST,) * 4,
        out_shape=tuple(
            pltpu.VMEM(shape, BF16) for shape in (qkv, qkv, (half, model), (half, model))
        ),
        compiler_params=pltpu.CompilerParams(vmem_limit_bytes=20 * 1024 * 1024),
    )(where, *held((*parts, embed, own, far)), gain.reshape(1, -1))


def attend_mine(embedded, own_qkv, far_qkv, own, far, up, down):
    return pl.pallas_call(
        attend_mine_kernel,
        in_specs=[FAST] * 5 + [SLOW] * 2,
        out_specs=(FAST,) * 3,
        out_shape=(
            pltpu.VMEM(embedded.shape, F32),
            pltpu.VMEM(up.shape, BF16),
            pltpu.VMEM(down.shape, BF16),
        ),
        scratch_shapes=[pltpu.SemaphoreType.DMA((2,))],
        compiler_params=pltpu.CompilerParams(vmem_limit_bytes=12 * 1024 * 1024),
    )(
        *held((own_qkv, far_qkv, embedded, own, far)),
        *(pltpu.with_memory_space_constraint(x, pltpu.HBM) for x in (up, down)),
    )


def join_kernel(mine, other, gain, after_attn, normed2):
    after = mine[...] + other[...].astype(F32)
    after_attn[...] = after
    normed2[...] = norm_rows(after, gain[...]).astype(BF16)


def join(mine, other, gain):
    return pl.pallas_call(
        join_kernel,
        in_specs=[FAST] * 3,
        out_specs=(FAST, FAST),
        out_shape=(pltpu.VMEM(mine.shape, F32), pltpu.VMEM(mine.shape, BF16)),
        compiler_params=SMALL,
    )(*held((mine, other)), gain)


def gelu(values):
    return 0.5 * values * (1.0 + lax.erf(values * 0.5 ** 0.5))


def feed_through(normed, up, down):
    return dot(gelu(dot(normed, up)).astype(BF16), down)


def own_kernel(normed, up, down, feed):
    feed[...] = feed_through(normed[...], up[...], down[...])


def first_kernel(normed, up, down, part, feed):
    feed[...] = part[...] + feed_through(normed[...], up[...], down[...])


def feed_first(body, *operands):
    return pl.pallas_call(
        body,
        in_specs=[FAST] * len(operands),
        out_specs=FAST,
        out_shape=pltpu.VMEM(operands[0].shape, F32),
        compiler_params=pltpu.CompilerParams(vmem_limit_bytes=16 * 1024 * 1024),
    )(*held(operands))


def second_kernel(normed, up_far, down_far, up_own, down_own, near, opposite):
    part = feed_through(normed[...], up_far[...], down_far[...])
    part = part + feed_through(normed[...], up_own[...], down_own[...])
    quarter = near.shape[0]
    near[...] = part[:quarter].astype(BF16)
    opposite[...] = part[quarter:].astype(BF16)


def feed_second(*operands):
    half, model = operands[0].shape
    return pl.pallas_call(
        second_kernel,
        in_specs=[FAST] * 5,
        out_specs=(FAST, FAST),
        out_shape=(pltpu.VMEM((half // 2, model), BF16), pltpu.VMEM((half // 2, model), BF16)),
        compiler_params=pltpu.CompilerParams(vmem_limit_bytes=16 * 1024 * 1024),
    )(*held(operands))


def layer(
    candidates,
    owner_row,
    selected,
    dest_slot,
    patch_weight,
    positions,
    qkv_weight,
    out_weight,
    attn_gain,
    mlp_gain,
    up_weight,
    down_weight,
):
    groups = lax.axis_size("mp")
    group = lax.axis_index("mp")
    pair = group // 2
    quarter = candidates.shape[1]
    where = jnp.stack([lax.axis_index("dp") % SPREAD, group]).astype(jnp.int32)

    outgoing, senders, mlp_piece = route(
        owner_row, selected, dest_slot, candidates, up_weight, down_weight
    )
    incoming = lax.all_to_all(outgoing, "dp", split_axis=0, concat_axis=0, tiled=True)

    pixel_width, width = patch_weight.shape
    model = out_weight.shape[1]
    embed_own = jnp.concatenate([patch_weight.T, positions.T], axis=1)
    attn_own = jnp.concatenate([qkv_weight.transpose(1, 2, 0).reshape(-1, model), out_weight])
    embed_piece, both_piece = copier(
        extract_kernel, ((width, UNIT), (4 * width, UNIT)), where, embed_own, attn_own
    )
    third = swap(embed_piece, "mp", 3)
    opposite = swap(both_piece, "mp", 2)
    neighbour = swap(embed_piece, "mp", 1)
    units = copier(units_kernel, ((6 * width, UNIT),), where, neighbour, opposite, third)[0]
    near = neighbours_of(units)
    far = [other_core(part) for part in near]
    shapes = ((groups * width, pixel_width + positions.shape[0]), attn_own.shape)
    placed = copier(place_attn_kernel, shapes, where, embed_own, *near, *far[:2])
    embed_whole, attn_far = copier(
        place_rest_kernel, shapes, where, *placed, *far[2:], aliases={1: 0, 2: 1}
    )
    mlp_piece = swap(mlp_piece, "mp", 2)
    near2 = neighbours_of(mlp_piece)
    rows2 = len(near2) * mlp_piece.shape[0]
    mine2 = copier(stack_kernel, ((rows2, model),), where, *near2)[0]
    far2 = other_core(mine2)
    up_far, down_far = copier(
        place_mlp_kernel, (up_weight.shape, down_weight.shape), where, mine2, far2
    )

    kept, given = choose(where, senders, incoming)
    third = swap(given, "mp", 3)
    opposite = swap(given, "mp", 2)
    neighbour = swap(kept, "mp", 1)
    own_qkv, far_qkv, embedded, other = attend(
        where, (kept, opposite, neighbour, third), embed_whole, attn_own, attn_far, attn_gain
    )
    other = swap(other, "mp", 1)
    mine, up_own, down_own = attend_mine(
        embedded, own_qkv, far_qkv, attn_own, attn_far, up_weight, down_weight
    )
    gain2 = widen(mlp_gain)
    after_attn, normed2 = join(mine, other, gain2)
    neighbour2 = swap(normed2, "mp", 1)
    feed = feed_first(own_kernel, normed2, up_own, down_own)
    feed = feed_first(first_kernel, normed2, up_far, down_far, feed)
    from_third = swap((after_attn + feed)[quarter:].astype(BF16), "mp", 3)
    for_near, for_opposite = feed_second(neighbour2, up_far, down_far, up_own, down_own)
    from_opposite = swap(for_opposite, "mp", 2)
    from_neighbour = swap(for_near, "mp", 1)
    kept_out = (after_attn[:quarter] + (feed[:quarter] + from_neighbour.astype(F32))).astype(BF16)
    given_out = (from_opposite.astype(F32) + from_third.astype(F32)).astype(BF16)
    swapped = pair == 1
    return jnp.stack(
        [jnp.where(swapped, given_out, kept_out), jnp.where(swapped, kept_out, given_out)]
    )


def solution(mesh):
    return jax.shard_map(
        layer,
        mesh=mesh,
        in_specs=(
            P("dp", "mp", None),
            P(),
            P(),
            P(),
            P(None, "mp"),
            P(None, "mp"),
            P(None, None, "mp"),
            P("mp", None),
            P(),
            P(),
            P(None, "mp"),
            P("mp", None),
        ),
        out_specs=P("dp", "mp", None),
        check_vma=False,
    )
```
